32 devices in a mesh: pool: 4 (over y, core), ga: 8 (over z, x).
Axes of the slice: x: 2, y: 2, z: 4, core: 2. Of those that a mesh axis runs over, the one named last changes fastest.
Arguments:
- coefficients: bfloat16 [4, 256, 2, 256, 128], P('pool', 'ga'), may hold values from -6 to 6
- stick_count: int32 [4, 8], P('pool', 'ga'), may hold values from 28 to 32, as said below
- dest_device: int32 [4, 256], P('pool', 'ga'), may hold values from -1 to 7, as said below
- dest_slot: int32 [4, 256], P('pool', 'ga'), may hold values from -1 to 31, as said below
- source_stick: int32 [4, 256], P('pool', 'ga'), may hold values from -1 to 255, as said below
Outputs:
- margins: float32 [4, 2, 256, 256], P('pool', None, 'ga')
The draws below stay inside these ranges and needn't reach their ends.
Inputs may be any that keep to these rules, and one draw needn't show every extreme that they name: Every k-point has a device whose 32 slots are all live; a device's live sticks are its first stick_count slots. `dest_device`: -1 exactly for sticks that land nowhere (among them all sticks that are not live); no device sends more than 8 of its sticks to one device, and some pair of devices reaches 8 for every k-point. `dest_slot`: -1 where dest_device is -1; the slots named are live slots of the layout of k-point q-1, no slot named twice. `source_stick`: the exact inverse of dest_device and dest_slot: a slot names a stick exactly when that stick names the slot, else -1.
All inputs are finite; a program needn't handle non-finite values.
Results may differ from the reference program's by a relative error of at most 0.0003.
Values may be sent and summed in bfloat16 or wider, within the bound.
A program may use at most 64 MiB of HBM per device.

```python
import jax
import jax.numpy as jnp
from jax import lax

NB = 256
PW = 128
SLOTS = 32
KPTS = 4
STICKS = 256
CAP = 8
N_GA = 8


def stick_maps(key):
    base_key = jax.random.fold_in(key, 7101)
    subkeys = jax.random.split(base_key, 6)
    lowest = SLOTS - max(1, SLOTS // 8)
    counts = jax.random.randint(subkeys[0], (KPTS, N_GA), lowest, SLOTS + 1)
    shifts = jax.random.randint(subkeys[1], (KPTS,), 0, N_GA)
    offsets = jax.vmap(lambda sub: jax.random.permutation(sub, N_GA))(jax.random.split(subkeys[2], KPTS))
    dest_order = jax.vmap(lambda sub: jax.random.permutation(sub, SLOTS))(jax.random.split(subkeys[3], KPTS * N_GA)).reshape(KPTS, N_GA, SLOTS)
    source_order = jax.vmap(lambda sub: jax.random.permutation(sub, SLOTS))(jax.random.split(subkeys[4], KPTS * N_GA)).reshape(KPTS, N_GA, SLOTS)
    full_dest = jax.random.randint(subkeys[5], (KPTS,), 0, N_GA)
    kpoint_list = jnp.arange(KPTS)
    counts = counts.at[(kpoint_list - 1) % KPTS, full_dest].set(SLOTS)
    full_source = (full_dest + shifts + offsets[:, 0]) % N_GA
    counts = counts.at[kpoint_list, full_source].set(SLOTS)
    shape = (KPTS, N_GA, SLOTS)
    device_grid = jnp.broadcast_to(jnp.arange(N_GA)[None, :, None], shape)
    kpoint_grid = jnp.broadcast_to(kpoint_list[:, None, None], shape)
    block_of = jnp.arange(SLOTS) // CAP
    chosen = offsets[:, block_of][:, None, :]
    source_dev = (device_grid + shifts[:, None, None] + chosen) % N_GA
    source_slot = jnp.take_along_axis(source_order, source_dev, axis=1)
    prev_counts = jnp.roll(counts, 1, axis=0)
    dest_live = dest_order < prev_counts[:, :, None]
    source_counts = jnp.take_along_axis(counts, source_dev.reshape(KPTS, N_GA * SLOTS), axis=1).reshape(shape)
    source_live = source_slot < source_counts
    valid = dest_live & source_live
    empty = jnp.full(shape, -1, jnp.int32)
    source_stick = empty.at[kpoint_grid, device_grid, dest_order].set(jnp.where(valid, source_dev * SLOTS + source_slot, -1).astype(jnp.int32))
    dest_device = empty.at[kpoint_grid, source_dev, source_slot].set(jnp.where(valid, device_grid, -1).astype(jnp.int32))
    dest_slot = empty.at[kpoint_grid, source_dev, source_slot].set(jnp.where(valid, dest_order, -1).astype(jnp.int32))
    flat_shape = (KPTS, N_GA * SLOTS)
    return (counts.astype(jnp.int32), dest_device.reshape(flat_shape), dest_slot.reshape(flat_shape), source_stick.reshape(flat_shape))


def draw_stick_count(key, part):
    return stick_maps(key)[0]


def draw_dest_device(key, part):
    return stick_maps(key)[1]


def draw_dest_slot(key, part):
    return stick_maps(key)[2]


def draw_source_stick(key, part):
    return stick_maps(key)[3]


def block_scale(own_key, dims, cuts, low, top_value):
    def one(position, shards_of):
        heights = jax.random.uniform(jax.random.fold_in(jax.random.fold_in(own_key, 6), position), (shards_of,), jnp.float32, low / len(cuts), top_value / len(cuts))
        return jnp.repeat(jnp.exp(heights), dims[position] // shards_of).reshape((-1,) + (1,) * (len(dims) - position - 1))

    gain = one(*cuts[0])
    for cut in cuts[1:]:
        gain = gain * one(*cut)
    return gain


def noise(own_key, extent, width, bound, pieces=(), kind=jnp.bfloat16):
    array = jax.random.normal(own_key, extent, jnp.float32) * width
    if len(pieces) > 0:
        array = block_scale(own_key, extent, pieces, -0.22, 0.18) * array
    return jnp.clip(array, min=-bound, max=bound).astype(kind)


def setup_inputs(seed: int = 0) -> dict:
    streams_of = jax.random.split(jax.random.key(seed), 6)
    coefficients = noise(streams_of[0], (KPTS, STICKS, 2, NB, PW), 1.0, 6.0, ((0, 4), (1, 8)))
    stick_count = draw_stick_count(jax.random.fold_in(streams_of[5], 71), 0)
    dest_device = draw_dest_device(jax.random.fold_in(streams_of[5], 71), 0)
    dest_slot = draw_dest_slot(jax.random.fold_in(streams_of[5], 71), 0)
    source_stick = draw_source_stick(jax.random.fold_in(streams_of[5], 71), 0)
    return {"coefficients": coefficients, "stick_count": stick_count, "dest_device": dest_device, "dest_slot": dest_slot, "source_stick": source_stick}


def reference(coefficients, stick_count, dest_device, dest_slot, source_stick):
    norm_scale = jnp.float32((2 * STICKS * PW) ** -0.5)
    slot_index = (jnp.arange(STICKS) % SLOTS).astype(jnp.int32)
    owner_device = (jnp.arange(STICKS) // SLOTS).astype(jnp.int32)
    results = []
    for kpoint in range(KPTS):
        neighbour = (kpoint + 1) % KPTS
        live_mask = slot_index < stick_count[kpoint][owner_device]
        bra_rows = jnp.where(live_mask[:, None, None, None], coefficients[kpoint], 0).astype(jnp.float32)
        anchor = source_stick[neighbour]
        safe_index = jnp.clip(anchor, 0, STICKS - 1).astype(jnp.int32)
        agreeing = (anchor >= 0) & (dest_device[neighbour][safe_index] == owner_device) & (dest_slot[neighbour][safe_index] == slot_index)
        ket_rows = jnp.where(agreeing[:, None, None, None], coefficients[neighbour][safe_index], 0).astype(jnp.float32)
        swapped = jnp.stack([ket_rows[:, 1], -ket_rows[:, 0]], axis=1)
        real_part = jnp.einsum('scmg,scng->mn', bra_rows, ket_rows, precision=lax.Precision.HIGHEST)
        imag_part = jnp.einsum('scmg,scng->mn', bra_rows, swapped, precision=lax.Precision.HIGHEST)
        results.append(jnp.stack([real_part, imag_part]) * norm_scale)
    return jnp.stack(results)
```

```python
import functools

import jax
import jax.numpy as jnp
from jax import lax
from jax.experimental import pallas as pl
from jax.experimental.pallas import tpu as pltpu
from jax.sharding import PartitionSpec as P

MESH = pl.DeviceIdType.MESH
HALVES = 2


def flipped(me, r):
    value = me
    bit = 1
    while bit <= r:
        if r & bit:
            value = value + bit * (1 - 2 * lax.rem(me // bit, 2))
        bit *= 2
    return value


def kernel(
    scale, coef, count, source, out,
    stage, send, mine, theirs_a, theirs_b, ket, acc, rs, near_map, far_map, live_count, slot_map,
    load_sem, own_sem, send_sem, recv_sem, fsend_sem, frecv_sem,
    map_send, map_recv, fmap_send, fmap_recv, map_sem, count_sem, rs_send, rs_recv,
):
    groups, pools = lax.axis_size("ga"), lax.axis_size("pool")
    me, pool = lax.axis_index("ga"), lax.axis_index("pool")
    prev, succ = lax.rem(pool + pools - 1, pools), lax.rem(pool + 1, pools)
    slots, _, bands, waves = stage.shape
    depth = 2 * waves // groups // HALVES
    width = depth // 2
    half = bands // 2
    rows = bands // groups
    lead = slots // 2
    theirs = (theirs_a, theirs_b)
    chunks = [(0, 0, lead), (0, lead, lead), (1, 0, lead), (1, lead, lead // 2), (1, lead + lead // 2, lead // 2)]
    order = [1] + [r for d in range(1, groups // 2) for r in (2 * d + 1, 2 * d)]
    near = [r for r in order if r < groups // 2]
    far = [r for r in order if r >= groups // 2]

    def load(part):
        span = pl.ds(part * lead, lead)
        return pltpu.make_async_copy(coef.at[0, span], stage.at[span], load_sem.at[part])

    def own(c):
        h, first, size = chunks[c]
        return pltpu.make_async_copy(
            send.at[h, me, pl.ds(first, size)],
            mine.at[h, pl.ds(me * slots + first, size)],
            own_sem.at[c],
        )

    def exchange(c, r):
        h, first, size = chunks[c]
        dest = flipped(me, r)
        return pltpu.make_async_remote_copy(
            src_ref=send.at[h, dest, pl.ds(first, size)],
            dst_ref=mine.at[h, pl.ds(me * slots + first, size)],
            send_sem=send_sem.at[c, r],
            recv_sem=recv_sem.at[c, r],
            device_id={"ga": dest},
            device_id_type=MESH,
        )

    def forward(c, r):
        h, first, size = chunks[c]
        span = pl.ds(flipped(me, r) * slots + first, size)
        return pltpu.make_async_remote_copy(
            src_ref=mine.at[h, span],
            dst_ref=theirs[h].at[span],
            send_sem=fsend_sem.at[c, r],
            recv_sem=frecv_sem.at[c, r],
            device_id={"pool": prev},
            device_id_type=MESH,
        )

    def map_copy(r):
        dest = flipped(me, r)
        return pltpu.make_async_remote_copy(
            src_ref=near_map.at[me],
            dst_ref=near_map.at[me],
            send_sem=map_send.at[r],
            recv_sem=map_recv.at[r],
            device_id={"ga": dest},
            device_id_type=MESH,
        )

    def map_forward():
        return pltpu.make_async_remote_copy(
            src_ref=near_map,
            dst_ref=far_map,
            send_sem=fmap_send,
            recv_sem=fmap_recv,
            device_id={"pool": prev},
            device_id_type=MESH,
        )

    own_count = pltpu.make_async_copy(count, live_count, count_sem)
    own_count.start()
    for part in range(2):
        load(part).start()
    own_map = pltpu.make_async_copy(source, near_map.at[me], map_sem)
    own_map.start()

    barrier = pltpu.get_barrier_semaphore()
    for r in order:
        pl.semaphore_signal(barrier, inc=1, device_id={"ga": flipped(me, r)}, device_id_type=MESH)
    for other in (prev, succ):
        pl.semaphore_signal(barrier, inc=1, device_id={"pool": other}, device_id_type=MESH)

    def transposed(part):
        load(part).wait()

        def one(slot, carry):
            live = slot < live_count[0, 0]
            for k in range(2):
                block = stage[slot, k]
                block = jnp.where(live, block, jnp.zeros_like(block)).T
                block = block.reshape(HALVES, groups, width, bands)
                for h in range(HALVES):
                    send[h, :, slot, k * width:(k + 1) * width, :] = block[h]
            return carry

        lax.fori_loop(part * lead, (part + 1) * lead, one, 0)

    own_count.wait()
    transposed(0)
    own_map.wait()
    pl.semaphore_wait(barrier, groups + 1)
    for c in (0, 2):
        for r in near:
            exchange(c, r).start()
    for r in far:
        exchange(0, r).start()
    for r in order:
        map_copy(r).start()
    transposed(1)
    for c in (1, 3, 4):
        for r in near:
            exchange(c, r).start()
    for c in (1, 2, 3, 4):
        for r in far:
            exchange(c, r).start()
    for c in range(len(chunks)):
        own(c).start()
    for c in range(len(chunks)):
        own(c).wait()
        forward(c, 0).start()
    acc[...] = jnp.zeros_like(acc)

    def pass_on(c, steps):
        for r in steps:
            exchange(c, r).wait_recv()
            forward(c, r).start()

    for c in (0, 2, 1, 3, 4):
        pass_on(c, near)
    for r in order:
        map_copy(r).wait()
    map_forward().start()
    for c in (0, 1):
        pass_on(c, far)
    map_forward().wait()
    to_scalar = pltpu.make_async_copy(far_map, slot_map, map_sem)
    to_scalar.start()
    to_scalar.wait()

    def gather(h, b):
        for s in range(slots):
            index = slot_map[b, 0, s]
            block = theirs[h][jnp.maximum(index, 0)]
            block = jnp.where(index >= 0, block, jnp.zeros_like(block))
            span = pl.ds((b * slots + s) * depth, depth)
            ket[span, 0:bands] = block
            ket[span, bands:2 * bands] = jnp.concatenate([block[width:], -block[:width]], axis=0)

    def product(h, b, first, size):
        bra = mine[h, pl.ds(b * slots, slots), :, pl.ds(first, size)].reshape(slots * depth, size)
        other = ket[pl.ds(b * slots * depth, slots * depth), :]
        value = lax.dot_general(
            bra, other, (((0,), (0,)), ((), ())), preferred_element_type=jnp.float32
        )
        acc[pl.ds(first, size), :] += value

    def arrived(cs):
        for c in cs:
            for r in range(groups):
                forward(c, r).wait_recv()

    pass_on(2, far)
    arrived((0, 1))

    def first_half(b, carry):
        gather(0, b)
        product(0, b, 0, bands)
        return carry

    lax.fori_loop(0, groups, first_half, 0)
    for c in (3, 4):
        pass_on(c, far)
    arrived((2, 3, 4))

    near_half = me // (groups // 2)
    far_half = 1 - near_half
    far_first = pl.multiple_of(far_half * half, half)
    near_first = pl.multiple_of(near_half * half, half)

    def far_step(b, carry):
        gather(1, b)
        product(1, b, far_first, half)
        return carry

    lax.fori_loop(0, groups, far_step, 0)

    def piece(dest):
        return pltpu.make_async_remote_copy(
            src_ref=acc.at[pl.ds(dest * rows, rows)],
            dst_ref=rs.at[me],
            send_sem=rs_send.at[dest],
            recv_sem=rs_recv.at[me],
            device_id={"ga": dest},
            device_id_type=MESH,
        )

    def landed(origin):
        return pltpu.make_async_remote_copy(
            src_ref=acc.at[pl.ds(origin * rows, rows)],
            dst_ref=rs.at[origin],
            send_sem=rs_send.at[origin],
            recv_sem=rs_recv.at[origin],
            device_id={"ga": origin},
            device_id_type=MESH,
        )

    product(1, 0, near_first, half)
    mates = groups // 2
    for j in range(mates):
        piece(far_half * mates + lax.rem(me + j, mates)).start()

    def near_step(b, carry):
        product(1, b, near_first, half)
        return carry

    lax.fori_loop(1, groups, near_step, 0)
    total = acc[pl.ds(me * rows, rows), :]
    rs[pl.ds(me, 1)] = total[None]
    for j in range(1, mates):
        piece(near_half * mates + lax.rem(me + j, mates)).start()
    for r in range(1, groups):
        landed(lax.rem(me + r, groups)).wait_recv()
    total = rs[0]
    for g in range(1, groups):
        total = total + rs[g]
    total = total * scale
    out[0, 0] = total[:, :bands]
    out[0, 1] = total[:, bands:]

    for c in range(len(chunks)):
        for r in range(groups):
            forward(c, r).wait_send()
        for r in order:
            exchange(c, r).wait_send()
    for r in range(1, groups):
        landed(lax.rem(me + r, groups)).wait_send()


def in_one_kernel(coefficients, stick_count, dest_device, dest_slot, source_stick):
    groups = lax.axis_size("ga")
    _, slots, _, bands, waves = coefficients.shape
    depth = 2 * waves // groups // HALVES
    sticks = groups * slots
    rows = bands // groups
    scale = (2 * sticks * waves) ** (-0.5)
    any_space = pl.BlockSpec(memory_space=pl.ANY)
    sems = pltpu.SemaphoreType.DMA
    grid_sems = sems((5, groups))
    return pl.pallas_call(
        functools.partial(kernel, scale),
        out_shape=jax.ShapeDtypeStruct((1, 2, rows, bands), jnp.float32),
        in_specs=[any_space, any_space, any_space],
        out_specs=pl.BlockSpec(memory_space=pltpu.VMEM),
        scratch_shapes=[
            pltpu.VMEM((slots, 2, bands, waves), coefficients.dtype),
            pltpu.VMEM((HALVES, groups, slots, depth, bands), coefficients.dtype),
            pltpu.VMEM((HALVES, sticks, depth, bands), coefficients.dtype),
            pltpu.VMEM((sticks, depth, bands), coefficients.dtype),
            pltpu.VMEM((sticks, depth, bands), coefficients.dtype),
            pltpu.VMEM((sticks * depth, 2 * bands), coefficients.dtype),
            pltpu.VMEM((bands, 2 * bands), jnp.float32),
            pltpu.VMEM((groups, rows, 2 * bands), jnp.float32),
            pltpu.VMEM((groups, 1, slots), jnp.int32),
            pltpu.VMEM((groups, 1, slots), jnp.int32),
            pltpu.SMEM((1, 1), jnp.int32),
            pltpu.SMEM((groups, 1, slots), jnp.int32),
            sems((2,)), sems((5,)),
            grid_sems, grid_sems, grid_sems, grid_sems,
            sems((groups,)), sems((groups,)), sems, sems, sems, sems,
            sems((groups,)), sems((groups,)),
        ],
        compiler_params=pltpu.CompilerParams(collective_id=0, has_side_effects=True, vmem_limit_bytes=60 * 1024 * 1024),
    )(coefficients, stick_count, source_stick)


def passed_along(value, axis, steps):
    count = lax.axis_size(axis)
    pairs = [(source, (source + steps) % count) for source in range(count)]
    return lax.ppermute(value, axis, pairs)


def with_collectives(coefficients, stick_count, dest_device, dest_slot, source_stick):
    groups = lax.axis_size("ga")
    slot_count = coefficients.shape[1]
    bands = coefficients.shape[3]
    plane_waves = coefficients.shape[4]
    width = plane_waves // groups
    sticks = groups * slot_count
    norm_scale = (2 * groups * slot_count * plane_waves) ** (-0.5)
    split = coefficients[0].reshape(slot_count, 2, bands, groups, width)
    split = split.transpose(3, 0, 1, 4, 2)
    mine = lax.all_to_all(split, "ga", split_axis=0, concat_axis=0, tiled=True)
    mine = mine.reshape(sticks, 2 * width * bands)
    theirs = passed_along(mine, "pool", -1)
    anchor = passed_along(source_stick[0], "pool", -1)
    slot_list = jnp.arange(slot_count, dtype=jnp.int32)
    anchor = jnp.where(slot_list < stick_count[0, 0], anchor, -1)
    anchors = lax.all_gather(anchor, "ga", tiled=True)
    placer = (anchors[:, None] == jnp.arange(sticks, dtype=jnp.int32)[None, :]).astype(jnp.bfloat16)
    ket = jnp.dot(placer, theirs, preferred_element_type=jnp.float32).astype(jnp.bfloat16)
    bra = mine.reshape(sticks, 2, width, bands)
    ket = ket.reshape(sticks, 2, width, bands)
    swapped = jnp.stack([ket[:, 1], -ket[:, 0]], axis=1)
    real_part = jnp.einsum("scgm,scgn->mn", bra, ket, preferred_element_type=jnp.float32)
    imag_part = jnp.einsum("scgm,scgn->mn", bra, swapped, preferred_element_type=jnp.float32)
    partial_value = jnp.stack([real_part, imag_part])
    owned = lax.psum_scatter(partial_value, "ga", scatter_dimension=1, tiled=True)
    return (owned * norm_scale)[None]


def local(coefficients, *rest):
    groups = lax.axis_size("ga")
    width = coefficients.shape[4] // groups
    if width % 16 == 0 and coefficients.shape[1] % 8 == 0 and groups & (groups - 1) == 0:
        return in_one_kernel(coefficients, *rest)
    return with_collectives(coefficients, *rest)


def solution(mesh):
    return jax.shard_map(
        local,
        mesh=mesh,
        in_specs=(
            P("pool", "ga", None, None, None),
            P("pool", "ga"),
            P("pool", "ga"),
            P("pool", "ga"),
            P("pool", "ga"),
        ),
        out_specs=P("pool", None, "ga", None),
        check_vma=False,
    )
```

```python
import functools

import jax
import jax.numpy as jnp
from jax import lax
from jax.experimental import pallas as pl
from jax.experimental.pallas import tpu as pltpu
from jax.sharding import PartitionSpec as P

MESH = pl.DeviceIdType.MESH
HALVES = 2


def flipped(me, r):
    value = me
    bit = 1
    while bit <= r:
        if r & bit:
            value = value + bit * (1 - 2 * lax.rem(me // bit, 2))
        bit *= 2
    return value


def kernel(
    scale, coef, count, source, out,
    stage, send, mine, theirs_a, theirs_b, ket, acc, rs, leaving, entered, near_map, far_map, live_count, slot_map,
    load_sem, own_sem, send_sem, recv_sem, fsend_sem, frecv_sem,
    map_send, map_recv, fmap_send, fmap_recv, map_sem, count_sem, rs_send, rs_recv, cross_send, cross_recv, gate,
):
    groups, pools = lax.axis_size("ga"), lax.axis_size("pool")
    me, pool = lax.axis_index("ga"), lax.axis_index("pool")
    prev, succ = lax.rem(pool + pools - 1, pools), lax.rem(pool + 1, pools)
    slots, _, bands, waves = stage.shape
    depth = 2 * waves // groups // HALVES
    width = depth // 2
    half = bands // 2
    rows = bands // groups
    lead = slots // 2
    theirs = (theirs_a, theirs_b)
    chunks = [(0, 0, lead), (0, lead, lead), (1, 0, lead), (1, lead, lead // 2), (1, lead + lead // 2, lead // 2)]
    order = [1] + [r for d in range(1, groups // 2) for r in (2 * d + 1, 2 * d)]
    near = [r for r in order if r < groups // 2]
    far = [r for r in order if r >= groups // 2]

    late = [c for c in range(len(chunks)) if chunks[c][0] > 0]
    second = lax.rem(pool, 2) == 1
    first = lax.rem(pool, 2) == 0

    def load(part):
        span = pl.ds(part * lead, lead)
        return pltpu.make_async_copy(coef.at[0, span], stage.at[span], load_sem.at[part])

    def own(c):
        h, first, size = chunks[c]
        return pltpu.make_async_copy(
            send.at[h, me, pl.ds(first, size)],
            mine.at[h, pl.ds(me * slots + first, size)],
            own_sem.at[c],
        )

    def exchange(c, r):
        h, first, size = chunks[c]
        dest = flipped(me, r)
        return pltpu.make_async_remote_copy(
            src_ref=send.at[h, dest, pl.ds(first, size)],
            dst_ref=mine.at[h, pl.ds(me * slots + first, size)],
            send_sem=send_sem.at[c, r],
            recv_sem=recv_sem.at[c, r],
            device_id={"ga": dest},
            device_id_type=MESH,
        )

    def forward(c, r):
        h, first, size = chunks[c]
        span = pl.ds(flipped(me, r) * slots + first, size)
        return pltpu.make_async_remote_copy(
            src_ref=mine.at[h, span],
            dst_ref=theirs[h].at[span],
            send_sem=fsend_sem.at[c, r],
            recv_sem=frecv_sem.at[c, r],
            device_id={"pool": prev},
            device_id_type=MESH,
        )

    def map_copy(r):
        dest = flipped(me, r)
        return pltpu.make_async_remote_copy(
            src_ref=near_map.at[me],
            dst_ref=near_map.at[me],
            send_sem=map_send.at[r],
            recv_sem=map_recv.at[r],
            device_id={"ga": dest},
            device_id_type=MESH,
        )

    def map_forward():
        return pltpu.make_async_remote_copy(
            src_ref=near_map,
            dst_ref=far_map,
            send_sem=fmap_send,
            recv_sem=fmap_recv,
            device_id={"pool": prev},
            device_id_type=MESH,
        )

    own_count = pltpu.make_async_copy(count, live_count, count_sem)
    own_count.start()
    for part in range(2):
        load(part).start()
    own_map = pltpu.make_async_copy(source, near_map.at[me], map_sem)
    own_map.start()

    barrier = pltpu.get_barrier_semaphore()
    for r in order:
        pl.semaphore_signal(barrier, inc=1, device_id={"ga": flipped(me, r)}, device_id_type=MESH)
    for other in (prev, succ):
        pl.semaphore_signal(barrier, inc=1, device_id={"pool": other}, device_id_type=MESH)

    def transposed(part):
        load(part).wait()

        def one(slot, carry):
            live = slot < live_count[0, 0]
            for k in range(2):
                block = stage[slot, k]
                block = jnp.where(live, block, jnp.zeros_like(block)).T
                block = block.reshape(HALVES, groups, width, bands)
                for h in range(HALVES):
                    send[h, :, slot, k * width:(k + 1) * width, :] = block[h]
            return carry

        lax.fori_loop(part * lead, (part + 1) * lead, one, 0)

    own_count.wait()
    transposed(0)
    own_map.wait()
    pl.semaphore_wait(barrier, groups + 1)
    for c in (0, 2):
        for r in near:
            exchange(c, r).start()
    for r in far:
        exchange(0, r).start()
    for r in order:
        map_copy(r).start()
    transposed(1)
    for c in (1, 3, 4):
        for r in near:
            exchange(c, r).start()
    for r in far:
        exchange(1, r).start()

    def late_sends():
        for c in late:
            for r in far:
                exchange(c, r).start()

    pl.when(first)(late_sends)
    for c in range(len(chunks)):
        own(c).start()
    for c in range(len(chunks)):
        own(c).wait()
        forward(c, 0).start()
    acc[...] = jnp.zeros_like(acc)

    def pass_on(c, steps):
        for r in steps:
            exchange(c, r).wait_recv()
            forward(c, r).start()

    for c in (0, 2, 1, 3, 4):
        pass_on(c, near)
    for r in order:
        map_copy(r).wait()
    map_forward().start()
    for c in (0, 1):
        pass_on(c, far)
    map_forward().wait()
    to_scalar = pltpu.make_async_copy(far_map, slot_map, map_sem)
    to_scalar.start()
    to_scalar.wait()

    def gather(h, b):
        for s in range(slots):
            index = slot_map[b, 0, s]
            block = theirs[h][jnp.maximum(index, 0)]
            block = jnp.where(index >= 0, block, jnp.zeros_like(block))
            span = pl.ds((b * slots + s) * depth, depth)
            ket[span, 0:bands] = block
            ket[span, bands:2 * bands] = jnp.concatenate([block[width:], -block[:width]], axis=0)

    def product(h, b, first, size):
        bra = mine[h, pl.ds(b * slots, slots), :, pl.ds(first, size)].reshape(slots * depth, size)
        other = ket[pl.ds(b * slots * depth, slots * depth), :]
        value = lax.dot_general(
            bra, other, (((0,), (0,)), ((), ())), preferred_element_type=jnp.float32
        )
        acc[pl.ds(first, size), :] += value

    def arrived(cs):
        for c in cs:
            for r in range(groups):
                forward(c, r).wait_recv()

    @pl.when(second)
    def _():
        pl.semaphore_wait(gate, 1)
        late_sends()

    pass_on(2, far)

    @pl.when(first)
    def _():
        for c in (0, 1, 2):
            for r in far:
                exchange(c, r).wait_send()
        pl.semaphore_signal(gate, inc=1, device_id={"pool": succ}, device_id_type=MESH)

    arrived((0, 1))

    def first_half(b, carry):
        gather(0, b)
        product(0, b, 0, bands)
        return carry

    lax.fori_loop(0, groups, first_half, 0)
    for c in (3, 4):
        pass_on(c, far)
    arrived((2, 3, 4))

    near_half = me // (groups // 2)
    far_half = 1 - near_half
    far_first = pl.multiple_of(far_half * half, half)
    near_first = pl.multiple_of(near_half * half, half)

    def far_step(b, carry):
        gather(1, b)
        product(1, b, far_first, half)
        return carry

    lax.fori_loop(0, groups, far_step, 0)

    mates = groups // 2
    base = near_half * mates
    seat = me - base
    across = lax.rem(me + mates, groups)

    def partial_sum(side, part, j, outgoing):
        dest = base + lax.rem(seat + (j if outgoing else mates - j), mates)
        block = lax.rem(dest + side * mates, groups)
        columns = pl.ds(part * bands, bands)
        return pltpu.make_async_remote_copy(
            src_ref=acc.at[pl.ds(block * rows, rows), columns],
            dst_ref=rs.at[side, j, :, columns],
            send_sem=rs_send.at[side, part, j],
            recv_sem=rs_recv.at[side, part, j],
            device_id={"ga": dest},
            device_id_type=MESH,
        )

    def crossing(part):
        columns = pl.ds(part * bands, bands)
        return pltpu.make_async_remote_copy(
            src_ref=leaving.at[:, columns],
            dst_ref=entered.at[:, columns],
            send_sem=cross_send.at[part],
            recv_sem=cross_recv.at[part],
            device_id={"ga": across},
            device_id_type=MESH,
        )

    def send_partials(side):
        for part in range(2):
            for j in range(1, mates):
                partial_sum(side, part, j, True).start()

    def summed(side, part):
        columns = pl.ds(part * bands, bands)
        block = lax.rem(me + side * mates, groups)
        value = acc[pl.ds(pl.multiple_of(block * rows, rows), rows), columns]
        for j in range(1, mates):
            partial_sum(side, part, j, False).wait_recv()
            value = value + rs[side, j, :, columns]
        return value

    send_partials(1)

    def near_step(b, carry):
        product(1, b, near_first, half)
        return carry

    lax.fori_loop(0, groups, near_step, 0)
    send_partials(0)
    for part in range(2):
        leaving[:, pl.ds(part * bands, bands)] = summed(1, part)
        crossing(part).start()
    for part in range(2):
        value = summed(0, part)
        crossing(part).wait_recv()
        value = value + entered[:, pl.ds(part * bands, bands)]
        out[0, part] = value * scale

    for c in range(len(chunks)):
        for r in range(groups):
            forward(c, r).wait_send()
        for r in near:
            exchange(c, r).wait_send()
    for c in (3, 4):
        for r in far:
            exchange(c, r).wait_send()

    @pl.when(second)
    def _():
        for c in (0, 1, 2):
            for r in far:
                exchange(c, r).wait_send()

    for side in range(2):
        for part in range(2):
            for j in range(1, mates):
                partial_sum(side, part, j, True).wait_send()
    for part in range(2):
        crossing(part).wait_send()


def in_one_kernel(coefficients, stick_count, dest_device, dest_slot, source_stick):
    groups = lax.axis_size("ga")
    _, slots, _, bands, waves = coefficients.shape
    depth = 2 * waves // groups // HALVES
    sticks = groups * slots
    rows = bands // groups
    scale = (2 * sticks * waves) ** (-0.5)
    any_space = pl.BlockSpec(memory_space=pl.ANY)
    sems = pltpu.SemaphoreType.DMA
    grid_sems = sems((5, groups))
    return pl.pallas_call(
        functools.partial(kernel, scale),
        out_shape=jax.ShapeDtypeStruct((1, 2, rows, bands), jnp.float32),
        in_specs=[any_space, any_space, any_space],
        out_specs=pl.BlockSpec(memory_space=pltpu.VMEM),
        scratch_shapes=[
            pltpu.VMEM((slots, 2, bands, waves), coefficients.dtype),
            pltpu.VMEM((HALVES, groups, slots, depth, bands), coefficients.dtype),
            pltpu.VMEM((HALVES, sticks, depth, bands), coefficients.dtype),
            pltpu.VMEM((sticks, depth, bands), coefficients.dtype),
            pltpu.VMEM((sticks, depth, bands), coefficients.dtype),
            pltpu.VMEM((sticks * depth, 2 * bands), coefficients.dtype),
            pltpu.VMEM((bands, 2 * bands), jnp.float32),
            pltpu.VMEM((2, groups // 2, rows, 2 * bands), jnp.float32),
            pltpu.VMEM((rows, 2 * bands), jnp.float32),
            pltpu.VMEM((rows, 2 * bands), jnp.float32),
            pltpu.VMEM((groups, 1, slots), jnp.int32),
            pltpu.VMEM((groups, 1, slots), jnp.int32),
            pltpu.SMEM((1, 1), jnp.int32),
            pltpu.SMEM((groups, 1, slots), jnp.int32),
            sems((2,)), sems((5,)),
            grid_sems, grid_sems, grid_sems, grid_sems,
            sems((groups,)), sems((groups,)), sems, sems, sems, sems,
            sems((2, 2, groups // 2)), sems((2, 2, groups // 2)), sems((2,)), sems((2,)), pltpu.SemaphoreType.REGULAR,
        ],
        compiler_params=pltpu.CompilerParams(collective_id=0, has_side_effects=True, vmem_limit_bytes=60 * 1024 * 1024),
    )(coefficients, stick_count, source_stick)


def passed_along(value, axis, steps):
    count = lax.axis_size(axis)
    pairs = [(source, (source + steps) % count) for source in range(count)]
    return lax.ppermute(value, axis, pairs)


def with_collectives(coefficients, stick_count, dest_device, dest_slot, source_stick):
    groups = lax.axis_size("ga")
    slot_count = coefficients.shape[1]
    bands = coefficients.shape[3]
    plane_waves = coefficients.shape[4]
    width = plane_waves // groups
    sticks = groups * slot_count
    norm_scale = (2 * groups * slot_count * plane_waves) ** (-0.5)
    split = coefficients[0].reshape(slot_count, 2, bands, groups, width)
    split = split.transpose(3, 0, 1, 4, 2)
    mine = lax.all_to_all(split, "ga", split_axis=0, concat_axis=0, tiled=True)
    mine = mine.reshape(sticks, 2 * width * bands)
    theirs = passed_along(mine, "pool", -1)
    anchor = passed_along(source_stick[0], "pool", -1)
    slot_list = jnp.arange(slot_count, dtype=jnp.int32)
    anchor = jnp.where(slot_list < stick_count[0, 0], anchor, -1)
    anchors = lax.all_gather(anchor, "ga", tiled=True)
    placer = (anchors[:, None] == jnp.arange(sticks, dtype=jnp.int32)[None, :]).astype(jnp.bfloat16)
    ket = jnp.dot(placer, theirs, preferred_element_type=jnp.float32).astype(jnp.bfloat16)
    bra = mine.reshape(sticks, 2, width, bands)
    ket = ket.reshape(sticks, 2, width, bands)
    swapped = jnp.stack([ket[:, 1], -ket[:, 0]], axis=1)
    real_part = jnp.einsum("scgm,scgn->mn", bra, ket, preferred_element_type=jnp.float32)
    imag_part = jnp.einsum("scgm,scgn->mn", bra, swapped, preferred_element_type=jnp.float32)
    partial_value = jnp.stack([real_part, imag_part])
    owned = lax.psum_scatter(partial_value, "ga", scatter_dimension=1, tiled=True)
    return (owned * norm_scale)[None]


def local(coefficients, *rest):
    groups = lax.axis_size("ga")
    width = coefficients.shape[4] // groups
    if width % 16 == 0 and coefficients.shape[1] % 8 == 0 and groups & (groups - 1) == 0 and lax.axis_size("pool") % 2 == 0:
        return in_one_kernel(coefficients, *rest)
    return with_collectives(coefficients, *rest)


def solution(mesh):
    return jax.shard_map(
        local,
        mesh=mesh,
        in_specs=(
            P("pool", "ga", None, None, None),
            P("pool", "ga"),
            P("pool", "ga"),
            P("pool", "ga"),
            P("pool", "ga"),
        ),
        out_specs=P("pool", None, "ga", None),
        check_vma=False,
    )
```

```python
import functools

import jax
import jax.numpy as jnp
from jax import lax
from jax.experimental import pallas as pl
from jax.experimental.pallas import tpu as pltpu
from jax.sharding import PartitionSpec as P

MESH = pl.DeviceIdType.MESH
HALVES = 2
CHUNKS = 6


def flipped(me, r):
    value = me
    bit = 1
    while bit <= r:
        if r & bit:
            value = value + bit * (1 - 2 * lax.rem(me // bit, 2))
        bit *= 2
    return value


def kernel(
    scale, coef, count, device, slot, source, out,
    stage, send, mine_a, mine_b, theirs_a, theirs_b, picked, ket, acc, rs, leaving, entered,
    maps, near_map, far_map, live_count, slot_map,
    load_sem, own_sem, send_sem, recv_sem, fsend_sem, frecv_sem,
    map_send, map_recv, fmap_send, fmap_recv, map_sem, count_sem,
    rs_send, rs_recv, cross_send, cross_recv, gate,
):
    groups, pools = lax.axis_size("ga"), lax.axis_size("pool")
    me, pool = lax.axis_index("ga"), lax.axis_index("pool")
    prev, succ = lax.rem(pool + pools - 1, pools), lax.rem(pool + 1, pools)
    slots, _, bands, waves = stage.shape
    depth = 2 * waves // groups // HALVES
    width = depth // 2
    half = bands // 2
    rows = bands // groups
    mine, theirs = (mine_a, mine_b), (theirs_a, theirs_b)
    quarter = slots // 4
    chunks = [
        (0, 0, quarter), (0, quarter, quarter), (0, 2 * quarter, 2 * quarter),
        (1, 0, 2 * quarter), (1, 2 * quarter, quarter), (1, 3 * quarter, quarter),
    ]
    early, late = (0, 1, 2), (3, 4, 5)
    order = [1] + [r for d in range(1, groups // 2) for r in (2 * d + 1, 2 * d)]
    near = [r for r in order if r < groups // 2]
    far = [r for r in order if r >= groups // 2]
    second = lax.rem(pool, 2) == 1
    first = lax.rem(pool, 2) == 0

    def load(part):
        span = pl.ds(part * quarter, quarter)
        return pltpu.make_async_copy(coef.at[0, span], stage.at[span], load_sem.at[part])

    def own(c):
        h, start, size = chunks[c]
        return pltpu.make_async_copy(
            send.at[h, me, pl.ds(start, size)], mine[h].at[me, pl.ds(start, size)], own_sem.at[c]
        )

    def exchange(c, r):
        h, start, size = chunks[c]
        dest = flipped(me, r)
        return pltpu.make_async_remote_copy(
            src_ref=send.at[h, dest, pl.ds(start, size)],
            dst_ref=mine[h].at[me, pl.ds(start, size)],
            send_sem=send_sem.at[c, r],
            recv_sem=recv_sem.at[c, r],
            device_id={"ga": dest},
            device_id_type=MESH,
        )

    def forward(c, r):
        h, start, size = chunks[c]
        origin = flipped(me, r)
        return pltpu.make_async_remote_copy(
            src_ref=mine[h].at[origin, pl.ds(start, size)],
            dst_ref=theirs[h].at[origin, pl.ds(start, size)],
            send_sem=fsend_sem.at[c, r],
            recv_sem=frecv_sem.at[c, r],
            device_id={"pool": prev},
            device_id_type=MESH,
        )

    def map_copy(r):
        dest = flipped(me, r)
        return pltpu.make_async_remote_copy(
            src_ref=near_map.at[me],
            dst_ref=near_map.at[me],
            send_sem=map_send.at[r],
            recv_sem=map_recv.at[r],
            device_id={"ga": dest},
            device_id_type=MESH,
        )

    def map_forward():
        return pltpu.make_async_remote_copy(
            src_ref=near_map,
            dst_ref=far_map,
            send_sem=fmap_send,
            recv_sem=fmap_recv,
            device_id={"pool": prev},
            device_id_type=MESH,
        )

    own_count = pltpu.make_async_copy(count, live_count, count_sem)
    own_count.start()
    for part in range(4):
        load(part).start()
    own_maps = [
        pltpu.make_async_copy(ref, maps.at[n], map_sem.at[n])
        for n, ref in enumerate((device, slot, source))
    ]
    for copy in own_maps:
        copy.start()

    barrier = pltpu.get_barrier_semaphore()
    for r in order:
        pl.semaphore_signal(barrier, inc=1, device_id={"ga": flipped(me, r)}, device_id_type=MESH)
    for other in (prev, succ):
        pl.semaphore_signal(barrier, inc=1, device_id={"pool": other}, device_id_type=MESH)

    def transposed(part):
        load(part).wait()

        def one(place, carry):
            live = place < live_count[0, 0]
            for k in range(2):
                block = stage[place, k]
                block = jnp.where(live, block, jnp.zeros_like(block)).T
                block = block.reshape(HALVES, groups, width, bands)
                for h in range(HALVES):
                    send[h, :, place, k * width:(k + 1) * width, :] = block[h]
            return carry

        lax.fori_loop(part * quarter, (part + 1) * quarter, one, 0)

    def send_off(cs, steps):
        for c in cs:
            for r in steps:
                exchange(c, r).start()

    own_count.wait()
    transposed(0)
    for copy in own_maps:
        copy.wait()
    landing = jnp.where(maps[0] >= 0, maps[0] * slots + maps[1], -1)
    near_map[pl.ds(me, 1)] = jnp.where(second, landing, maps[2])[None]
    pl.semaphore_wait(barrier, groups + 1)
    send_off((0,), near)
    for r in order:
        map_copy(r).start()
    send_off((0,), far)
    transposed(1)
    send_off((1, 3), near)
    send_off((1,), far)
    transposed(2)
    transposed(3)
    send_off((2, 4, 5), near)
    send_off((2,), far)
    pl.when(first)(functools.partial(send_off, late, far))

    for c in range(CHUNKS):
        own(c).start()
    for c in range(CHUNKS):
        own(c).wait()
        forward(c, 0).start()
    acc[...] = jnp.zeros_like(acc)

    def pass_on(c, steps):
        for r in steps:
            exchange(c, r).wait_recv()
            forward(c, r).start()

    def arrived(c):
        for r in range(groups):
            forward(c, r).wait_recv()

    for c in (0, 1, 3, 2, 4, 5):
        pass_on(c, near)
    for r in order:
        map_copy(r).wait()
    map_forward().start()
    for c in early:
        pass_on(c, far)
    map_forward().wait()
    to_scalar = pltpu.make_async_copy(far_map, slot_map, map_sem.at[0])
    to_scalar.start()
    to_scalar.wait()

    @pl.when(first)
    def _():
        pass_on(3, far)
        for c in (0, 1, 2, 3):
            for r in far:
                exchange(c, r).wait_send()
        pl.semaphore_signal(gate, inc=1, device_id={"pool": succ}, device_id_type=MESH)

    @pl.when(second)
    def _():
        pl.semaphore_wait(gate, 1)
        send_off(late, far)

    def looked_up(ref, b, s):
        index = slot_map[b, 0, s]
        place = jnp.maximum(index, 0)
        block = ref[place // slots, lax.rem(place, slots)]
        return jnp.where(index >= 0, block, jnp.zeros_like(block))

    def put_ket(b, s, block):
        ket[b, s, :, 0:bands] = block
        ket[b, s, :, bands:2 * bands] = jnp.concatenate([block[width:], -block[:width]], axis=0)

    def gather_bra(h):
        def step(b, carry):
            for s in range(slots):
                picked[b, s] = looked_up(mine[h], b, s)
            return carry

        lax.fori_loop(0, groups, step, 0)

    def gather_ket(h):
        def step(b, carry):
            for s in range(slots):
                put_ket(b, s, looked_up(theirs[h], b, s))
            return carry

        lax.fori_loop(0, groups, step, 0)

    def plain_ket(c):
        h, start, size = chunks[c]

        def step(b, carry):
            for s in range(start, start + size):
                put_ket(b, s, theirs[h][b, s])
            return carry

        lax.fori_loop(0, groups, step, 0)

    def product(bra, c, row, many):
        _, start, size = chunks[c]
        span = groups * quarter // 2 // size

        def step(i, carry):
            some = pl.ds(i * span, span)
            left = bra[some, pl.ds(start, size), :, pl.ds(row, many)].reshape(span * size * depth, many)
            right = ket[some, pl.ds(start, size)].reshape(span * size * depth, 2 * bands)
            acc[pl.ds(row, many), :] += lax.dot_general(
                left, right, (((0,), (0,)), ((), ())), preferred_element_type=jnp.float32
            )
            return carry

        lax.fori_loop(0, groups // span, step, 0)

    near_half = me // (groups // 2)
    far_row = pl.multiple_of((1 - near_half) * half, half)
    near_row = pl.multiple_of(near_half * half, half)
    last = late[-1]

    @pl.when(first)
    def _():
        gather_bra(0)
        for c in early:
            arrived(c)
            plain_ket(c)
            product(picked, c, 0, bands)
        for c in late[1:]:
            pass_on(c, far)
        gather_bra(1)
        for c in late[:-1]:
            arrived(c)
            plain_ket(c)
            product(picked, c, 0, bands)
        arrived(last)
        plain_ket(last)
        product(picked, last, far_row, half)

    @pl.when(second)
    def _():
        for c in early:
            arrived(c)
        gather_ket(0)
        for c in early:
            product(mine[0], c, 0, bands)
        pass_on(late[0], far)
        for c in late:
            arrived(c)
        gather_ket(1)
        product(mine[1], late[0], 0, bands)
        pass_on(late[1], far)
        product(mine[1], late[1], 0, bands)
        pass_on(last, far)
        product(mine[1], last, far_row, half)

    mates = groups // 2
    base = near_half * mates
    seat = me - base
    across = lax.rem(me + mates, groups)

    def partial_sum(side, part, j, outgoing):
        dest = base + lax.rem(seat + (j if outgoing else mates - j), mates)
        block = lax.rem(dest + side * mates, groups)
        columns = pl.ds(part * bands, bands)
        return pltpu.make_async_remote_copy(
            src_ref=acc.at[pl.ds(block * rows, rows), columns],
            dst_ref=rs.at[side, j, :, columns],
            send_sem=rs_send.at[side, part, j],
            recv_sem=rs_recv.at[side, part, j],
            device_id={"ga": dest},
            device_id_type=MESH,
        )

    def crossing(part):
        columns = pl.ds(part * bands, bands)
        return pltpu.make_async_remote_copy(
            src_ref=leaving.at[:, columns],
            dst_ref=entered.at[:, columns],
            send_sem=cross_send.at[part],
            recv_sem=cross_recv.at[part],
            device_id={"ga": across},
            device_id_type=MESH,
        )

    def send_partials(side):
        for part in range(2):
            for j in range(1, mates):
                partial_sum(side, part, j, True).start()

    def summed(side, part):
        columns = pl.ds(part * bands, bands)
        block = lax.rem(me + side * mates, groups)
        value = acc[pl.ds(pl.multiple_of(block * rows, rows), rows), columns]
        for j in range(1, mates):
            partial_sum(side, part, j, False).wait_recv()
            value = value + rs[side, j, :, columns]
        return value

    send_partials(1)
    pl.when(first)(functools.partial(product, picked, last, near_row, half))
    pl.when(second)(functools.partial(product, mine[1], last, near_row, half))
    send_partials(0)
    for c in range(CHUNKS):
        for r in range(groups):
            forward(c, r).wait_send()
        for r in near:
            exchange(c, r).wait_send()
    for c in late[1:]:
        for r in far:
            exchange(c, r).wait_send()

    @pl.when(second)
    def _():
        for c in (0, 1, 2, 3):
            for r in far:
                exchange(c, r).wait_send()

    for part in range(2):
        leaving[:, pl.ds(part * bands, bands)] = summed(1, part)
        crossing(part).start()
    for part in range(2):
        value = summed(0, part)
        crossing(part).wait_recv()
        value = value + entered[:, pl.ds(part * bands, bands)]
        out[0, part] = value * scale

    for side in range(2):
        for part in range(2):
            for j in range(1, mates):
                partial_sum(side, part, j, True).wait_send()
    for part in range(2):
        crossing(part).wait_send()


def in_one_kernel(coefficients, stick_count, dest_device, dest_slot, source_stick):
    groups = lax.axis_size("ga")
    _, slots, _, bands, waves = coefficients.shape
    depth = 2 * waves // groups // HALVES
    sticks = groups * slots
    rows = bands // groups
    scale = (2 * sticks * waves) ** (-0.5)
    any_space = pl.BlockSpec(memory_space=pl.ANY)
    sems = pltpu.SemaphoreType.DMA
    grid_sems = sems((CHUNKS, groups))
    exchanged = pltpu.VMEM((groups, slots, depth, bands), coefficients.dtype)
    return pl.pallas_call(
        functools.partial(kernel, scale),
        out_shape=jax.ShapeDtypeStruct((1, 2, rows, bands), jnp.float32),
        in_specs=[any_space] * 5,
        out_specs=pl.BlockSpec(memory_space=pltpu.VMEM),
        scratch_shapes=[
            pltpu.VMEM((slots, 2, bands, waves), coefficients.dtype),
            pltpu.VMEM((HALVES, groups, slots, depth, bands), coefficients.dtype),
            exchanged, exchanged, exchanged, exchanged, exchanged,
            pltpu.VMEM((groups, slots, depth, 2 * bands), coefficients.dtype),
            pltpu.VMEM((bands, 2 * bands), jnp.float32),
            pltpu.VMEM((2, groups // 2, rows, 2 * bands), jnp.float32),
            pltpu.VMEM((rows, 2 * bands), jnp.float32),
            pltpu.VMEM((rows, 2 * bands), jnp.float32),
            pltpu.VMEM((3, 1, slots), jnp.int32),
            pltpu.VMEM((groups, 1, slots), jnp.int32),
            pltpu.VMEM((groups, 1, slots), jnp.int32),
            pltpu.SMEM((1, 1), jnp.int32),
            pltpu.SMEM((groups, 1, slots), jnp.int32),
            sems((4,)), sems((CHUNKS,)),
            grid_sems, grid_sems, grid_sems, grid_sems,
            sems((groups,)), sems((groups,)), sems, sems, sems((3,)), sems,
            sems((2, 2, groups // 2)), sems((2, 2, groups // 2)), sems((2,)), sems((2,)), pltpu.SemaphoreType.REGULAR,
        ],
        compiler_params=pltpu.CompilerParams(collective_id=0, has_side_effects=True, vmem_limit_bytes=60 * 1024 * 1024),
    )(coefficients, stick_count, dest_device, dest_slot, source_stick)


def passed_along(value, axis, steps):
    count = lax.axis_size(axis)
    pairs = [(source, (source + steps) % count) for source in range(count)]
    return lax.ppermute(value, axis, pairs)


def with_collectives(coefficients, stick_count, dest_device, dest_slot, source_stick):
    groups = lax.axis_size("ga")
    slot_count = coefficients.shape[1]
    bands = coefficients.shape[3]
    plane_waves = coefficients.shape[4]
    width = plane_waves // groups
    sticks = groups * slot_count
    norm_scale = (2 * groups * slot_count * plane_waves) ** (-0.5)
    split = coefficients[0].reshape(slot_count, 2, bands, groups, width)
    split = split.transpose(3, 0, 1, 4, 2)
    mine = lax.all_to_all(split, "ga", split_axis=0, concat_axis=0, tiled=True)
    mine = mine.reshape(sticks, 2 * width * bands)
    theirs = passed_along(mine, "pool", -1)
    anchor = passed_along(source_stick[0], "pool", -1)
    slot_list = jnp.arange(slot_count, dtype=jnp.int32)
    anchor = jnp.where(slot_list < stick_count[0, 0], anchor, -1)
    anchors = lax.all_gather(anchor, "ga", tiled=True)
    placer = (anchors[:, None] == jnp.arange(sticks, dtype=jnp.int32)[None, :]).astype(jnp.bfloat16)
    ket = jnp.dot(placer, theirs, preferred_element_type=jnp.float32).astype(jnp.bfloat16)
    bra = mine.reshape(sticks, 2, width, bands)
    ket = ket.reshape(sticks, 2, width, bands)
    swapped = jnp.stack([ket[:, 1], -ket[:, 0]], axis=1)
    real_part = jnp.einsum("scgm,scgn->mn", bra, ket, preferred_element_type=jnp.float32)
    imag_part = jnp.einsum("scgm,scgn->mn", bra, swapped, preferred_element_type=jnp.float32)
    partial_value = jnp.stack([real_part, imag_part])
    owned = lax.psum_scatter(partial_value, "ga", scatter_dimension=1, tiled=True)
    return (owned * norm_scale)[None]


def local(coefficients, *rest):
    groups = lax.axis_size("ga")
    width = coefficients.shape[4] // groups
    paired = groups & (groups - 1) == 0 and lax.axis_size("pool") % 2 == 0
    if paired and width % 16 == 0 and coefficients.shape[1] % 8 == 0:
        return in_one_kernel(coefficients, *rest)
    return with_collectives(coefficients, *rest)


def solution(mesh):
    return jax.shard_map(
        local,
        mesh=mesh,
        in_specs=(
            P("pool", "ga", None, None, None),
            P("pool", "ga"),
            P("pool", "ga"),
            P("pool", "ga"),
            P("pool", "ga"),
        ),
        out_specs=P("pool", None, "ga", None),
        check_vma=False,
    )
```

```python
import functools

import jax
import jax.numpy as jnp
from jax import lax
from jax.experimental import pallas as pl
from jax.experimental.pallas import tpu as pltpu
from jax.sharding import PartitionSpec as P

MESH = pl.DeviceIdType.MESH
HALVES = 2
CHUNKS = 6


def flipped(me, r):
    value = me
    bit = 1
    while bit <= r:
        if r & bit:
            value = value + bit * (1 - 2 * lax.rem(me // bit, 2))
        bit *= 2
    return value


def kernel(
    scale, coef, count, device, slot, source, out,
    stage, send, mine_a, mine_b, theirs_a, theirs_b, picked, ket, acc, rs, leaving, entered,
    maps, near_map, far_map, live_count, slot_map,
    load_sem, own_sem, send_sem, recv_sem, fsend_sem, frecv_sem,
    map_send, map_recv, fmap_send, fmap_recv, map_sem, count_sem,
    rs_send, rs_recv, cross_send, cross_recv, gate,
):
    groups, pools = lax.axis_size("ga"), lax.axis_size("pool")
    me, pool = lax.axis_index("ga"), lax.axis_index("pool")
    prev, succ = lax.rem(pool + pools - 1, pools), lax.rem(pool + 1, pools)
    slots, _, bands, waves = stage.shape
    depth = 2 * waves // groups // HALVES
    width = depth // 2
    half = bands // 2
    rows = bands // groups
    mine, theirs = (mine_a, mine_b), (theirs_a, theirs_b)
    quarter = slots // 4
    chunks = [
        (0, 0, quarter), (0, quarter, quarter), (0, 2 * quarter, 2 * quarter),
        (1, 0, 2 * quarter), (1, 2 * quarter, quarter), (1, 3 * quarter, quarter),
    ]
    early, late = (0, 1, 2), (3, 4, 5)
    order = [1] + [r for d in range(1, groups // 2) for r in (2 * d + 1, 2 * d)]
    near = [r for r in order if r < groups // 2]
    far = [r for r in order if r >= groups // 2]
    second = lax.rem(pool, 2) == 1
    first = lax.rem(pool, 2) == 0

    def load(part):
        span = pl.ds(part * quarter, quarter)
        return pltpu.make_async_copy(coef.at[0, span], stage.at[span], load_sem.at[part])

    def own(h):
        return pltpu.make_async_copy(send.at[h, me], mine[h].at[me], own_sem.at[h])

    def exchange(c, r):
        h, start, size = chunks[c]
        dest = flipped(me, r)
        return pltpu.make_async_remote_copy(
            src_ref=send.at[h, dest, pl.ds(start, size)],
            dst_ref=mine[h].at[me, pl.ds(start, size)],
            send_sem=send_sem.at[0 if r in near else c + 1],
            recv_sem=recv_sem.at[c, 0 if r in near else r - len(near)],
            device_id={"ga": dest},
            device_id_type=MESH,
        )

    def forward(c, r):
        h, start, size = chunks[c]
        origin = flipped(me, r)
        return pltpu.make_async_remote_copy(
            src_ref=mine[h].at[origin, pl.ds(start, size)],
            dst_ref=theirs[h].at[origin, pl.ds(start, size)],
            send_sem=fsend_sem.at[h],
            recv_sem=frecv_sem.at[c],
            device_id={"pool": prev},
            device_id_type=MESH,
        )

    def whole(ref, send_one, recv_one, axis, other):
        return pltpu.make_async_remote_copy(
            src_ref=ref, dst_ref=ref, send_sem=send_one, recv_sem=recv_one,
            device_id={axis: other}, device_id_type=MESH,
        )

    def near_received(c):
        h, start, size = chunks[c]
        ref = mine[h].at[pl.ds(0, len(near)), pl.ds(start, size)]
        whole(ref, send_sem.at[0], recv_sem.at[c, 0], "ga", flipped(me, 1)).wait_recv()

    def near_sent():
        ref = send.at[:, pl.ds(0, len(near))]
        whole(ref, send_sem.at[0], recv_sem.at[0, 0], "ga", flipped(me, 1)).wait_send()

    def forwards_sent():
        for h in range(HALVES):
            whole(mine[h], fsend_sem.at[h], frecv_sem.at[0], "pool", prev).wait_send()

    def far_sent(c):
        h, start, size = chunks[c]
        ref = send.at[h, pl.ds(0, len(far)), pl.ds(start, size)]
        whole(ref, send_sem.at[c + 1], recv_sem.at[c, 0], "ga", flipped(me, 1)).wait_send()

    def map_copy(r):
        dest = flipped(me, r)
        return pltpu.make_async_remote_copy(
            src_ref=near_map.at[me],
            dst_ref=near_map.at[me],
            send_sem=map_send,
            recv_sem=map_recv,
            device_id={"ga": dest},
            device_id_type=MESH,
        )

    def map_forward():
        return pltpu.make_async_remote_copy(
            src_ref=near_map,
            dst_ref=far_map,
            send_sem=fmap_send,
            recv_sem=fmap_recv,
            device_id={"pool": prev},
            device_id_type=MESH,
        )

    own_count = pltpu.make_async_copy(count, live_count, count_sem)
    own_count.start()
    for part in range(4):
        load(part).start()
    own_maps = [
        pltpu.make_async_copy(ref, maps.at[n], map_sem)
        for n, ref in enumerate((device, slot, source))
    ]
    for copy in own_maps:
        copy.start()

    barrier = pltpu.get_barrier_semaphore()
    for r in order:
        pl.semaphore_signal(barrier, inc=1, device_id={"ga": flipped(me, r)}, device_id_type=MESH)
    for other in (prev, succ):
        pl.semaphore_signal(barrier, inc=1, device_id={"pool": other}, device_id_type=MESH)

    def transposed(part):
        load(part).wait()

        def one(place, carry):
            live = place < live_count[0, 0]
            for k in range(2):
                block = stage[place, k]
                block = jnp.where(live, block, jnp.zeros_like(block)).T
                block = block.reshape(HALVES, groups, width, bands)
                for h in range(HALVES):
                    send[h, :, place, k * width:(k + 1) * width, :] = block[h]
            return carry

        lax.fori_loop(part * quarter, (part + 1) * quarter, one, 0)

    def send_off(cs, steps):
        for c in cs:
            for r in steps:
                exchange(c, r).start()

    own_count.wait()
    transposed(0)
    pltpu.make_async_copy(maps, maps, map_sem).wait()
    landing = jnp.where(maps[0] >= 0, maps[0] * slots + maps[1], -1)
    near_map[pl.ds(me, 1)] = jnp.where(second, landing, maps[2])[None]
    pl.semaphore_wait(barrier, groups + 1)
    send_off((0,), near)
    for r in order:
        map_copy(r).start()
    send_off((0,), far)
    transposed(1)
    send_off((1, 3), near)
    send_off((1,), far)
    transposed(2)
    transposed(3)
    send_off((2, 4, 5), near)
    send_off((2,), far)
    pl.when(first)(functools.partial(send_off, late, far))

    for h in range(HALVES):
        own(h).start()
    for h in range(HALVES):
        own(h).wait()
    for c in range(CHUNKS):
        forward(c, 0).start()
    acc[...] = jnp.zeros_like(acc)

    def pass_on(c, steps):
        for r in steps:
            exchange(c, r).wait_recv()
            forward(c, r).start()

    def arrived(c):
        h, start, size = chunks[c]
        ref = theirs[h].at[:, pl.ds(start, size)]
        whole(ref, fsend_sem.at[h], frecv_sem.at[c], "pool", prev).wait_recv()

    for c in (0, 1, 3, 2, 4, 5):
        near_received(c)
        for r in near:
            forward(c, r).start()
    every_map = whole(near_map.at[pl.ds(0, groups - 1)], map_send, map_recv, "ga", flipped(me, 1))
    every_map.wait_send()
    every_map.wait_recv()
    map_forward().start()
    for c in early:
        pass_on(c, far)
    map_forward().wait()
    to_scalar = pltpu.make_async_copy(far_map, slot_map, map_sem)
    to_scalar.start()
    to_scalar.wait()

    @pl.when(first)
    def _():
        pass_on(3, far)
        for c in (0, 1, 2, 3):
            far_sent(c)
        pl.semaphore_signal(gate, inc=1, device_id={"pool": succ}, device_id_type=MESH)

    @pl.when(second)
    def _():
        pl.semaphore_wait(gate, 1)
        send_off(late, far)

    def looked_up(ref, b, s):
        index = slot_map[b, 0, s]
        place = jnp.maximum(index, 0)
        block = ref[place // slots, lax.rem(place, slots)]
        return jnp.where(index >= 0, block, jnp.zeros_like(block))

    def put_ket(b, s, block):
        ket[b, s, :, 0:bands] = block
        ket[b, s, :, bands:2 * bands] = jnp.concatenate([block[width:], -block[:width]], axis=0)

    def gather_bra(h):
        def step(b, carry):
            for s in range(slots):
                picked[b, s] = looked_up(mine[h], b, s)
            return carry

        lax.fori_loop(0, groups, step, 0)

    def gather_ket(h):
        def step(b, carry):
            for s in range(slots):
                put_ket(b, s, looked_up(theirs[h], b, s))
            return carry

        lax.fori_loop(0, groups, step, 0)

    def plain_ket(c):
        h, start, size = chunks[c]

        def step(b, carry):
            for s in range(start, start + size):
                put_ket(b, s, theirs[h][b, s])
            return carry

        lax.fori_loop(0, groups, step, 0)

    def product(bra, c, row, many):
        _, start, size = chunks[c]
        span = groups * quarter // 2 // size

        def step(i, carry):
            some = pl.ds(i * span, span)
            left = bra[some, pl.ds(start, size), :, pl.ds(row, many)].reshape(span * size * depth, many)
            right = ket[some, pl.ds(start, size)].reshape(span * size * depth, 2 * bands)
            acc[pl.ds(row, many), :] += lax.dot_general(
                left, right, (((0,), (0,)), ((), ())), preferred_element_type=jnp.float32
            )
            return carry

        lax.fori_loop(0, groups // span, step, 0)

    near_half = me // (groups // 2)
    far_row = pl.multiple_of((1 - near_half) * half, half)
    near_row = pl.multiple_of(near_half * half, half)
    last = late[-1]

    @pl.when(first)
    def _():
        gather_bra(0)
        for c in early:
            arrived(c)
            plain_ket(c)
            product(picked, c, 0, bands)
        for c in late[1:]:
            pass_on(c, far)
        gather_bra(1)
        for c in late[:-1]:
            arrived(c)
            plain_ket(c)
            product(picked, c, 0, bands)
        arrived(last)
        plain_ket(last)
        product(picked, last, far_row, half)

    @pl.when(second)
    def _():
        for c in early:
            arrived(c)
        gather_ket(0)
        for c in early:
            product(mine[0], c, 0, bands)
        pass_on(late[0], far)
        for c in late:
            arrived(c)
        gather_ket(1)
        product(mine[1], late[0], 0, bands)
        pass_on(late[1], far)
        product(mine[1], late[1], 0, bands)
        pass_on(last, far)
        product(mine[1], last, far_row, half)

    mates = groups // 2
    base = near_half * mates
    seat = me - base
    across = lax.rem(me + mates, groups)

    def partial_sum(side, part, j):
        dest = base + lax.rem(seat + j, mates)
        block = lax.rem(dest + side * mates, groups)
        columns = pl.ds(part * bands, bands)
        return pltpu.make_async_remote_copy(
            src_ref=acc.at[pl.ds(block * rows, rows), columns],
            dst_ref=rs.at[side, j, :, columns],
            send_sem=rs_send,
            recv_sem=rs_recv.at[side, part],
            device_id={"ga": dest},
            device_id_type=MESH,
        )

    def crossing(part):
        columns = pl.ds(part * bands, bands)
        return pltpu.make_async_remote_copy(
            src_ref=leaving.at[:, columns],
            dst_ref=entered.at[:, columns],
            send_sem=cross_send,
            recv_sem=cross_recv.at[part],
            device_id={"ga": across},
            device_id_type=MESH,
        )

    def send_partials(side):
        for part in range(2):
            for j in range(1, mates):
                partial_sum(side, part, j).start()

    def summed(side, part):
        columns = pl.ds(part * bands, bands)
        block = lax.rem(me + side * mates, groups)
        value = acc[pl.ds(pl.multiple_of(block * rows, rows), rows), columns]
        ref = rs.at[side, pl.ds(1, mates - 1), :, columns]
        whole(ref, rs_send, rs_recv.at[side, part], "ga", across).wait_recv()
        for j in range(1, mates):
            value = value + rs[side, j, :, columns]
        return value

    send_partials(1)
    pl.when(first)(functools.partial(product, picked, last, near_row, half))
    pl.when(second)(functools.partial(product, mine[1], last, near_row, half))
    send_partials(0)
    forwards_sent()
    near_sent()
    for c in late[1:]:
        far_sent(c)

    @pl.when(second)
    def _():
        for c in (0, 1, 2, 3):
            far_sent(c)

    for part in range(2):
        leaving[:, pl.ds(part * bands, bands)] = summed(1, part)
        crossing(part).start()
    for part in range(2):
        value = summed(0, part)
        crossing(part).wait_recv()
        value = value + entered[:, pl.ds(part * bands, bands)]
        out[0, part] = value * scale

    whole(rs.at[:, pl.ds(1, mates - 1)], rs_send, rs_recv.at[0, 0], "ga", across).wait_send()
    whole(leaving, cross_send, cross_recv.at[0], "ga", across).wait_send()


def in_one_kernel(coefficients, stick_count, dest_device, dest_slot, source_stick):
    groups = lax.axis_size("ga")
    _, slots, _, bands, waves = coefficients.shape
    depth = 2 * waves // groups // HALVES
    sticks = groups * slots
    rows = bands // groups
    scale = (2 * sticks * waves) ** (-0.5)
    any_space = pl.BlockSpec(memory_space=pl.ANY)
    sems = pltpu.SemaphoreType.DMA
    exchanged = pltpu.VMEM((groups, slots, depth, bands), coefficients.dtype)
    return pl.pallas_call(
        functools.partial(kernel, scale),
        out_shape=pltpu.VMEM((1, 2, rows, bands), jnp.float32),
        in_specs=[any_space] * 5,
        out_specs=pl.BlockSpec(memory_space=pltpu.VMEM),
        scratch_shapes=[
            pltpu.VMEM((slots, 2, bands, waves), coefficients.dtype),
            pltpu.VMEM((HALVES, groups, slots, depth, bands), coefficients.dtype),
            exchanged, exchanged, exchanged, exchanged, exchanged,
            pltpu.VMEM((groups, slots, depth, 2 * bands), coefficients.dtype),
            pltpu.VMEM((bands, 2 * bands), jnp.float32),
            pltpu.VMEM((2, groups // 2, rows, 2 * bands), jnp.float32),
            pltpu.VMEM((rows, 2 * bands), jnp.float32),
            pltpu.VMEM((rows, 2 * bands), jnp.float32),
            pltpu.VMEM((3, 1, slots), jnp.int32),
            pltpu.VMEM((groups, 1, slots), jnp.int32),
            pltpu.VMEM((groups, 1, slots), jnp.int32),
            pltpu.SMEM((1, 1), jnp.int32),
            pltpu.SMEM((groups, 1, slots), jnp.int32),
            sems((4,)), sems((HALVES,)),
            sems((CHUNKS + 1,)), sems((CHUNKS, groups // 2 + 1)), sems((HALVES,)), sems((CHUNKS,)),
            sems, sems, sems, sems, sems, sems,
            sems, sems((2, 2)), sems, sems((2,)), pltpu.SemaphoreType.REGULAR,
        ],
        compiler_params=pltpu.CompilerParams(collective_id=0, has_side_effects=True, vmem_limit_bytes=60 * 1024 * 1024),
    )(coefficients, stick_count, dest_device, dest_slot, source_stick)


def passed_along(value, axis, steps):
    count = lax.axis_size(axis)
    pairs = [(source, (source + steps) % count) for source in range(count)]
    return lax.ppermute(value, axis, pairs)


def with_collectives(coefficients, stick_count, dest_device, dest_slot, source_stick):
    groups = lax.axis_size("ga")
    slot_count = coefficients.shape[1]
    bands = coefficients.shape[3]
    plane_waves = coefficients.shape[4]
    width = plane_waves // groups
    sticks = groups * slot_count
    norm_scale = (2 * groups * slot_count * plane_waves) ** (-0.5)
    split = coefficients[0].reshape(slot_count, 2, bands, groups, width)
    split = split.transpose(3, 0, 1, 4, 2)
    mine = lax.all_to_all(split, "ga", split_axis=0, concat_axis=0, tiled=True)
    mine = mine.reshape(sticks, 2 * width * bands)
    theirs = passed_along(mine, "pool", -1)
    anchor = passed_along(source_stick[0], "pool", -1)
    slot_list = jnp.arange(slot_count, dtype=jnp.int32)
    anchor = jnp.where(slot_list < stick_count[0, 0], anchor, -1)
    anchors = lax.all_gather(anchor, "ga", tiled=True)
    placer = (anchors[:, None] == jnp.arange(sticks, dtype=jnp.int32)[None, :]).astype(jnp.bfloat16)
    ket = jnp.dot(placer, theirs, preferred_element_type=jnp.float32).astype(jnp.bfloat16)
    bra = mine.reshape(sticks, 2, width, bands)
    ket = ket.reshape(sticks, 2, width, bands)
    swapped = jnp.stack([ket[:, 1], -ket[:, 0]], axis=1)
    real_part = jnp.einsum("scgm,scgn->mn", bra, ket, preferred_element_type=jnp.float32)
    imag_part = jnp.einsum("scgm,scgn->mn", bra, swapped, preferred_element_type=jnp.float32)
    partial_value = jnp.stack([real_part, imag_part])
    owned = lax.psum_scatter(partial_value, "ga", scatter_dimension=1, tiled=True)
    return (owned * norm_scale)[None]


def local(coefficients, *rest):
    groups = lax.axis_size("ga")
    width = coefficients.shape[4] // groups
    paired = groups & (groups - 1) == 0 and lax.axis_size("pool") % 2 == 0
    if paired and width % 16 == 0 and coefficients.shape[1] % 8 == 0:
        return in_one_kernel(coefficients, *rest)
    return with_collectives(coefficients, *rest)


def solution(mesh):
    return jax.shard_map(
        local,
        mesh=mesh,
        in_specs=(
            P("pool", "ga", None, None, None),
            P("pool", "ga"),
            P("pool", "ga"),
            P("pool", "ga"),
            P("pool", "ga"),
        ),
        out_specs=P("pool", None, "ga", None),
        check_vma=False,
    )
```

```python
import functools

import jax
import jax.numpy as jnp
from jax import lax
from jax.experimental import pallas as pl
from jax.experimental.pallas import tpu as pltpu
from jax.sharding import PartitionSpec as P

MESH = pl.DeviceIdType.MESH
HALVES = 2
CHUNKS = 5


def flipped(me, r):
    value = me
    bit = 1
    while bit <= r:
        if r & bit:
            value = value + bit * (1 - 2 * lax.rem(me // bit, 2))
        bit *= 2
    return value


def kernel(
    scale, coef, count, device, slot, source, out,
    stage, send, mine_a, mine_b, theirs_a, theirs_b, picked, ket, acc, rs, leaving, entered,
    maps, near_map, far_map, live_count, slot_map,
    load_sem, own_sem, send_sem, recv_sem, fsend_sem, frecv_sem,
    map_send, map_recv, fmap_send, fmap_recv, map_sem, count_sem,
    rs_send, rs_recv, cross_send, cross_recv, gate,
):
    groups, pools = lax.axis_size("ga"), lax.axis_size("pool")
    me, pool = lax.axis_index("ga"), lax.axis_index("pool")
    prev, succ = lax.rem(pool + pools - 1, pools), lax.rem(pool + 1, pools)
    slots, _, bands, waves = stage.shape
    depth = 2 * waves // groups // HALVES
    width = depth // 2
    half = bands // 2
    rows = bands // groups
    mine, theirs = (mine_a, mine_b), (theirs_a, theirs_b)
    quarter = slots // 4
    chunks = [
        (0, 0, quarter), (0, quarter, quarter), (0, 2 * quarter, 2 * quarter),
        (1, 0, 16), (1, 16, 16),
    ]
    early, late = (0, 1, 2), (3, 4)
    order = [1] + [r for d in range(1, groups // 2) for r in (2 * d + 1, 2 * d)]
    near = [r for r in order if r < groups // 2]
    far = [r for r in order if r >= groups // 2]
    second = lax.rem(pool, 2) == 1
    first = lax.rem(pool, 2) == 0

    def load(part):
        span = pl.ds(part * quarter, quarter)
        return pltpu.make_async_copy(coef.at[0, span], stage.at[span], load_sem.at[part])

    def own(h):
        return pltpu.make_async_copy(send.at[h, me], mine[h].at[me], own_sem.at[h])

    def exchange(c, r):
        h, start, size = chunks[c]
        dest = flipped(me, r)
        return pltpu.make_async_remote_copy(
            src_ref=send.at[h, dest, pl.ds(start, size)],
            dst_ref=mine[h].at[me, pl.ds(start, size)],
            send_sem=send_sem.at[0 if r in near else c + 1],
            recv_sem=recv_sem.at[c, 0 if r in near else r - len(near)],
            device_id={"ga": dest},
            device_id_type=MESH,
        )

    def forward(c, r):
        h, start, size = chunks[c]
        origin = flipped(me, r)
        return pltpu.make_async_remote_copy(
            src_ref=mine[h].at[origin, pl.ds(start, size)],
            dst_ref=theirs[h].at[origin, pl.ds(start, size)],
            send_sem=fsend_sem.at[h],
            recv_sem=frecv_sem.at[c],
            device_id={"pool": prev},
            device_id_type=MESH,
        )

    def whole(ref, send_one, recv_one, axis, other):
        return pltpu.make_async_remote_copy(
            src_ref=ref, dst_ref=ref, send_sem=send_one, recv_sem=recv_one,
            device_id={axis: other}, device_id_type=MESH,
        )

    def near_received(c):
        h, start, size = chunks[c]
        ref = mine[h].at[pl.ds(0, len(near)), pl.ds(start, size)]
        whole(ref, send_sem.at[0], recv_sem.at[c, 0], "ga", flipped(me, 1)).wait_recv()

    def near_sent():
        ref = send.at[:, pl.ds(0, len(near))]
        whole(ref, send_sem.at[0], recv_sem.at[0, 0], "ga", flipped(me, 1)).wait_send()

    def forwards_sent():
        for h in range(HALVES):
            whole(mine[h], fsend_sem.at[h], frecv_sem.at[0], "pool", prev).wait_send()

    def far_sent(c):
        h, start, size = chunks[c]
        ref = send.at[h, pl.ds(0, len(far)), pl.ds(start, size)]
        whole(ref, send_sem.at[c + 1], recv_sem.at[c, 0], "ga", flipped(me, 1)).wait_send()

    def map_copy(r):
        dest = flipped(me, r)
        return pltpu.make_async_remote_copy(
            src_ref=near_map.at[me],
            dst_ref=near_map.at[me],
            send_sem=map_send,
            recv_sem=map_recv,
            device_id={"ga": dest},
            device_id_type=MESH,
        )

    def map_forward():
        return pltpu.make_async_remote_copy(
            src_ref=near_map,
            dst_ref=far_map,
            send_sem=fmap_send,
            recv_sem=fmap_recv,
            device_id={"pool": prev},
            device_id_type=MESH,
        )

    own_count = pltpu.make_async_copy(count, live_count, count_sem)
    own_count.start()
    for part in range(4):
        load(part).start()
    own_maps = [
        pltpu.make_async_copy(ref, maps.at[n], map_sem)
        for n, ref in enumerate((device, slot, source))
    ]
    for copy in own_maps:
        copy.start()

    barrier = pltpu.get_barrier_semaphore()
    for r in order:
        pl.semaphore_signal(barrier, inc=1, device_id={"ga": flipped(me, r)}, device_id_type=MESH)
    for other in (prev, succ):
        pl.semaphore_signal(barrier, inc=1, device_id={"pool": other}, device_id_type=MESH)

    def transposed(part):
        load(part).wait()

        def one(place, carry):
            live = place < live_count[0, 0]
            for k in range(2):
                block = stage[place, k]
                block = jnp.where(live, block, jnp.zeros_like(block)).T
                block = block.reshape(HALVES, groups, width, bands)
                for h in range(HALVES):
                    send[h, :, place, k * width:(k + 1) * width, :] = block[h]
            return carry

        lax.fori_loop(part * quarter, (part + 1) * quarter, one, 0)

    def send_off(cs, steps):
        for c in cs:
            for r in steps:
                exchange(c, r).start()

    own_count.wait()
    transposed(0)
    pltpu.make_async_copy(maps, maps, map_sem).wait()
    landing = jnp.where(maps[0] >= 0, maps[0] * slots + maps[1], -1)
    near_map[pl.ds(me, 1)] = jnp.where(second, landing, maps[2])[None]
    pl.semaphore_wait(barrier, groups + 1)
    send_off((0,), near)
    for r in order:
        map_copy(r).start()
    send_off((0,), far)
    transposed(1)
    send_off((1, 3), near)
    send_off((1,), far)
    transposed(2)
    transposed(3)
    send_off((2, 4), near)
    send_off((2,), far)
    pl.when(first)(functools.partial(send_off, late, far))

    for h in range(HALVES):
        own(h).start()
    for h in range(HALVES):
        own(h).wait()

    for c in range(CHUNKS):
        forward(c, 0).start()
    acc[...] = jnp.zeros_like(acc)

    def pass_on(c, steps):
        for r in steps:
            exchange(c, r).wait_recv()
            forward(c, r).start()

    def arrived(c):
        h, start, size = chunks[c]
        ref = theirs[h].at[:, pl.ds(start, size)]
        whole(ref, fsend_sem.at[h], frecv_sem.at[c], "pool", prev).wait_recv()

    for c in (0, 1, 3, 2, 4):
        near_received(c)
        for r in near:
            forward(c, r).start()
    every_map = whole(near_map.at[pl.ds(0, groups - 1)], map_send, map_recv, "ga", flipped(me, 1))
    every_map.wait_send()
    every_map.wait_recv()
    map_forward().start()
    for c in early:
        pass_on(c, far)
    map_forward().wait()
    to_scalar = pltpu.make_async_copy(far_map, slot_map, map_sem)
    to_scalar.start()
    to_scalar.wait()

    @pl.when(first)
    def _():
        pass_on(3, far)
        for c in (0, 1, 2, 3):
            far_sent(c)
        pl.semaphore_signal(gate, inc=1, device_id={"pool": succ}, device_id_type=MESH)

    @pl.when(second)
    def _():
        pl.semaphore_wait(gate, 1)
        send_off(late, far)

    def looked_up(ref, b, s):
        index = slot_map[b, 0, s]
        place = jnp.maximum(index, 0)
        block = ref[place // slots, lax.rem(place, slots)]
        return jnp.where(index >= 0, block, jnp.zeros_like(block))

    def put_ket(b, s, block):
        ket[b, s, :, 0:bands] = block
        ket[b, s, :, bands:2 * bands] = jnp.concatenate([block[width:], -block[:width]], axis=0)

    def gather_bra(h):
        def step(b, carry):
            for s in range(slots):
                picked[b, s] = looked_up(mine[h], b, s)
            return carry

        lax.fori_loop(0, groups, step, 0)

    def gather_ket(h):
        def step(b, carry):
            for s in range(slots):
                put_ket(b, s, looked_up(theirs[h], b, s))
            return carry

        lax.fori_loop(0, groups, step, 0)

    def plain_ket(c):
        h, start, size = chunks[c]

        def step(b, carry):
            for s in range(start, start + size):
                put_ket(b, s, theirs[h][b, s])
            return carry

        lax.fori_loop(0, groups, step, 0)

    def product(bra, c, row, many):
        _, start, size = chunks[c]
        span = groups if many < bands else groups * quarter // 2 // size

        def step(i, carry):
            some = pl.ds(i * span, span)
            left = bra[some, pl.ds(start, size), :, pl.ds(row, many)].reshape(span * size * depth, many)
            right = ket[some, pl.ds(start, size)].reshape(span * size * depth, 2 * bands)
            acc[pl.ds(row, many), :] += lax.dot_general(
                left, right, (((0,), (0,)), ((), ())), preferred_element_type=jnp.float32
            )
            return carry

        lax.fori_loop(0, groups // span, step, 0)

    near_half = me // (groups // 2)
    far_row = pl.multiple_of((1 - near_half) * half, half)
    near_row = pl.multiple_of(near_half * half, half)

    @pl.when(first)
    def _():
        gather_bra(0)
        for c in early:
            arrived(c)
            plain_ket(c)
            product(picked, c, 0, bands)
        for c in late[1:]:
            pass_on(c, far)
        gather_bra(1)
        for c in late:
            arrived(c)
            plain_ket(c)
            product(picked, c, far_row, half)

    @pl.when(second)
    def _():
        for c in early:
            arrived(c)
        gather_ket(0)
        for c in early:
            product(mine[0], c, 0, bands)
        pass_on(late[0], far)
        for c in late:
            arrived(c)
        gather_ket(1)
        for c in late[1:]:
            pass_on(c, far)
        for c in late:
            product(mine[1], c, far_row, half)

    mates = groups // 2
    base = near_half * mates
    seat = me - base
    across = lax.rem(me + mates, groups)

    def partial_sum(side, part, j):
        dest = base + lax.rem(seat + j, mates)
        block = lax.rem(dest + side * mates, groups)
        columns = pl.ds(part * bands, bands)
        return pltpu.make_async_remote_copy(
            src_ref=acc.at[pl.ds(block * rows, rows), columns],
            dst_ref=rs.at[side, j, :, columns],
            send_sem=rs_send,
            recv_sem=rs_recv.at[side, part],
            device_id={"ga": dest},
            device_id_type=MESH,
        )

    def crossing(part):
        columns = pl.ds(part * bands, bands)
        return pltpu.make_async_remote_copy(
            src_ref=leaving.at[:, columns],
            dst_ref=entered.at[:, columns],
            send_sem=cross_send,
            recv_sem=cross_recv.at[part],
            device_id={"ga": across},
            device_id_type=MESH,
        )

    def send_partials(side):
        for part in range(2):
            for j in range(1, mates):
                partial_sum(side, part, j).start()

    def summed(side, part):
        columns = pl.ds(part * bands, bands)
        block = lax.rem(me + side * mates, groups)
        value = acc[pl.ds(pl.multiple_of(block * rows, rows), rows), columns]
        ref = rs.at[side, pl.ds(1, mates - 1), :, columns]
        whole(ref, rs_send, rs_recv.at[side, part], "ga", across).wait_recv()
        for j in range(1, mates):
            value = value + rs[side, j, :, columns]
        return value

    send_partials(1)

    def near_products(bra):
        for c in late:
            product(bra, c, near_row, half)

    pl.when(first)(functools.partial(near_products, picked))
    pl.when(second)(functools.partial(near_products, mine[1]))
    send_partials(0)
    forwards_sent()
    near_sent()
    for c in late[1:]:
        far_sent(c)

    @pl.when(second)
    def _():
        for c in (0, 1, 2, 3):
            far_sent(c)

    for part in range(2):
        leaving[:, pl.ds(part * bands, bands)] = summed(1, part)
        crossing(part).start()
    for part in range(2):
        value = summed(0, part)
        crossing(part).wait_recv()
        value = value + entered[:, pl.ds(part * bands, bands)]
        out[0, part] = value * scale

    whole(rs.at[:, pl.ds(1, mates - 1)], rs_send, rs_recv.at[0, 0], "ga", across).wait_send()
    whole(leaving, cross_send, cross_recv.at[0], "ga", across).wait_send()


def in_one_kernel(coefficients, stick_count, dest_device, dest_slot, source_stick):
    groups = lax.axis_size("ga")
    _, slots, _, bands, waves = coefficients.shape
    depth = 2 * waves // groups // HALVES
    sticks = groups * slots
    rows = bands // groups
    scale = (2 * sticks * waves) ** (-0.5)
    any_space = pl.BlockSpec(memory_space=pl.ANY)
    sems = pltpu.SemaphoreType.DMA
    exchanged = pltpu.VMEM((groups, slots, depth, bands), coefficients.dtype)
    return pl.pallas_call(
        functools.partial(kernel, scale),
        out_shape=pltpu.VMEM((1, 2, rows, bands), jnp.float32),
        in_specs=[any_space] * 5,
        out_specs=pl.BlockSpec(memory_space=pltpu.VMEM),
        scratch_shapes=[
            pltpu.VMEM((slots, 2, bands, waves), coefficients.dtype),
            pltpu.VMEM((HALVES, groups, slots, depth, bands), coefficients.dtype),
            exchanged, exchanged, exchanged, exchanged, exchanged,
            pltpu.VMEM((groups, slots, depth, 2 * bands), coefficients.dtype),
            pltpu.VMEM((bands, 2 * bands), jnp.float32),
            pltpu.VMEM((2, groups // 2, rows, 2 * bands), jnp.float32),
            pltpu.VMEM((rows, 2 * bands), jnp.float32),
            pltpu.VMEM((rows, 2 * bands), jnp.float32),
            pltpu.VMEM((3, 1, slots), jnp.int32),
            pltpu.VMEM((groups, 1, slots), jnp.int32),
            pltpu.VMEM((groups, 1, slots), jnp.int32),
            pltpu.SMEM((1, 1), jnp.int32),
            pltpu.SMEM((groups, 1, slots), jnp.int32),
            sems((4,)), sems((HALVES,)),
            sems((CHUNKS + 1,)), sems((CHUNKS, groups // 2 + 1)), sems((HALVES,)), sems((CHUNKS,)),
            sems, sems, sems, sems, sems, sems,
            sems, sems((2, 2)), sems, sems((2,)), pltpu.SemaphoreType.REGULAR,
        ],
        compiler_params=pltpu.CompilerParams(collective_id=0, has_side_effects=True, vmem_limit_bytes=60 * 1024 * 1024),
    )(coefficients, stick_count, dest_device, dest_slot, source_stick)


def passed_along(value, axis, steps):
    count = lax.axis_size(axis)
    pairs = [(source, (source + steps) % count) for source in range(count)]
    return lax.ppermute(value, axis, pairs)


def with_collectives(coefficients, stick_count, dest_device, dest_slot, source_stick):
    groups = lax.axis_size("ga")
    slot_count = coefficients.shape[1]
    bands = coefficients.shape[3]
    plane_waves = coefficients.shape[4]
    width = plane_waves // groups
    sticks = groups * slot_count
    norm_scale = (2 * groups * slot_count * plane_waves) ** (-0.5)
    split = coefficients[0].reshape(slot_count, 2, bands, groups, width)
    split = split.transpose(3, 0, 1, 4, 2)
    mine = lax.all_to_all(split, "ga", split_axis=0, concat_axis=0, tiled=True)
    mine = mine.reshape(sticks, 2 * width * bands)
    theirs = passed_along(mine, "pool", -1)
    anchor = passed_along(source_stick[0], "pool", -1)
    slot_list = jnp.arange(slot_count, dtype=jnp.int32)
    anchor = jnp.where(slot_list < stick_count[0, 0], anchor, -1)
    anchors = lax.all_gather(anchor, "ga", tiled=True)
    placer = (anchors[:, None] == jnp.arange(sticks, dtype=jnp.int32)[None, :]).astype(jnp.bfloat16)
    ket = jnp.dot(placer, theirs, preferred_element_type=jnp.float32).astype(jnp.bfloat16)
    bra = mine.reshape(sticks, 2, width, bands)
    ket = ket.reshape(sticks, 2, width, bands)
    swapped = jnp.stack([ket[:, 1], -ket[:, 0]], axis=1)
    real_part = jnp.einsum("scgm,scgn->mn", bra, ket, preferred_element_type=jnp.float32)
    imag_part = jnp.einsum("scgm,scgn->mn", bra, swapped, preferred_element_type=jnp.float32)
    partial_value = jnp.stack([real_part, imag_part])
    owned = lax.psum_scatter(partial_value, "ga", scatter_dimension=1, tiled=True)
    return (owned * norm_scale)[None]


def local(coefficients, *rest):
    groups = lax.axis_size("ga")
    width = coefficients.shape[4] // groups
    paired = groups & (groups - 1) == 0 and lax.axis_size("pool") % 2 == 0
    if paired and width % 16 == 0 and coefficients.shape[1] % 8 == 0:
        return in_one_kernel(coefficients, *rest)
    return with_collectives(coefficients, *rest)


def solution(mesh):
    return jax.shard_map(
        local,
        mesh=mesh,
        in_specs=(
            P("pool", "ga", None, None, None),
            P("pool", "ga"),
            P("pool", "ga"),
            P("pool", "ga"),
            P("pool", "ga"),
        ),
        out_specs=P("pool", None, "ga", None),
        check_vma=False,
    )
```

```python
import functools

import jax
import jax.numpy as jnp
from jax import lax
from jax.experimental import pallas as pl
from jax.experimental.pallas import tpu as pltpu
from jax.sharding import PartitionSpec as P

MESH = pl.DeviceIdType.MESH
HALVES = 2
CHUNKS = 5


def flipped(me, r):
    value = me
    bit = 1
    while bit <= r:
        if r & bit:
            value = value + bit * (1 - 2 * lax.rem(me // bit, 2))
        bit *= 2
    return value


def kernel(
    scale, coef, count, device, slot, source, out,
    stage, send, mine_a, mine_b, theirs_a, theirs_b, picked, ket, acc, rs, leaving, entered,
    maps, near_map, far_map, live_count, slot_map,
    load_sem, own_sem, send_sem, recv_sem, fsend_sem, frecv_sem,
    map_send, map_recv, fmap_send, fmap_recv, map_sem, count_sem,
    rs_send, rs_recv, cross_send, cross_recv, gate,
):
    groups, pools = lax.axis_size("ga"), lax.axis_size("pool")
    me, pool = lax.axis_index("ga"), lax.axis_index("pool")
    prev, succ = lax.rem(pool + pools - 1, pools), lax.rem(pool + 1, pools)
    slots, _, bands, waves = stage.shape
    depth = 2 * waves // groups
    width = depth // 2
    half = bands // 2
    rows = bands // groups
    mine, theirs = (mine_a, mine_b), (theirs_a, theirs_b)
    quarter = slots // 4
    chunks = [
        (0, 0, quarter), (0, quarter, quarter), (0, 2 * quarter, 2 * quarter),
        (1, 0, 3 * quarter), (1, 3 * quarter, quarter),
    ]
    early, late = (0, 1, 2), (3, 4)
    order = [1] + [r for d in range(1, groups // 2) for r in (2 * d + 1, 2 * d)]
    near = [r for r in order if r < groups // 2]
    far = [r for r in order if r >= groups // 2]
    second = lax.rem(pool, 2) == 1
    first = lax.rem(pool, 2) == 0

    def load(part):
        span = pl.ds(part * quarter, quarter)
        return pltpu.make_async_copy(coef.at[0, span], stage.at[span], load_sem.at[part])

    def own(h):
        return pltpu.make_async_copy(send.at[h, me], mine[h].at[me], own_sem.at[h])

    def exchange(c, r):
        h, start, size = chunks[c]
        dest = flipped(me, r)
        return pltpu.make_async_remote_copy(
            src_ref=send.at[h, dest, pl.ds(start, size)],
            dst_ref=mine[h].at[me, pl.ds(start, size)],
            send_sem=send_sem.at[0 if r in near else c + 1],
            recv_sem=recv_sem.at[c, 0 if r in near else r - len(near)],
            device_id={"ga": dest},
            device_id_type=MESH,
        )

    def forward(c, r):
        h, start, size = chunks[c]
        origin = flipped(me, r)
        return pltpu.make_async_remote_copy(
            src_ref=mine[h].at[origin, pl.ds(start, size)],
            dst_ref=theirs[h].at[origin, pl.ds(start, size)],
            send_sem=fsend_sem.at[h],
            recv_sem=frecv_sem.at[c],
            device_id={"pool": prev},
            device_id_type=MESH,
        )

    def whole(ref, send_one, recv_one, axis, other):
        return pltpu.make_async_remote_copy(
            src_ref=ref, dst_ref=ref, send_sem=send_one, recv_sem=recv_one,
            device_id={axis: other}, device_id_type=MESH,
        )

    def near_received(c):
        h, start, size = chunks[c]
        ref = mine[h].at[pl.ds(0, len(near)), pl.ds(start, size)]
        whole(ref, send_sem.at[0], recv_sem.at[c, 0], "ga", flipped(me, 1)).wait_recv()

    def near_sent():
        ref = send.at[:, pl.ds(0, len(near))]
        whole(ref, send_sem.at[0], recv_sem.at[0, 0], "ga", flipped(me, 1)).wait_send()

    def forwards_sent():
        for h in range(HALVES):
            whole(mine[h], fsend_sem.at[h], frecv_sem.at[0], "pool", prev).wait_send()

    def far_sent(c):
        h, start, size = chunks[c]
        ref = send.at[h, pl.ds(0, len(far)), pl.ds(start, size)]
        whole(ref, send_sem.at[c + 1], recv_sem.at[c, 0], "ga", flipped(me, 1)).wait_send()

    def map_copy(r):
        dest = flipped(me, r)
        return pltpu.make_async_remote_copy(
            src_ref=near_map.at[me],
            dst_ref=near_map.at[me],
            send_sem=map_send,
            recv_sem=map_recv,
            device_id={"ga": dest},
            device_id_type=MESH,
        )

    def map_forward():
        return pltpu.make_async_remote_copy(
            src_ref=near_map,
            dst_ref=far_map,
            send_sem=fmap_send,
            recv_sem=fmap_recv,
            device_id={"pool": prev},
            device_id_type=MESH,
        )

    own_count = pltpu.make_async_copy(count, live_count, count_sem)
    own_count.start()
    for part in range(4):
        load(part).start()
    own_maps = [
        pltpu.make_async_copy(ref, maps.at[n], map_sem)
        for n, ref in enumerate((device, slot, source))
    ]
    for copy in own_maps:
        copy.start()

    barrier = pltpu.get_barrier_semaphore()
    for r in order:
        pl.semaphore_signal(barrier, inc=1, device_id={"ga": flipped(me, r)}, device_id_type=MESH)
    for other in (prev, succ):
        pl.semaphore_signal(barrier, inc=1, device_id={"pool": other}, device_id_type=MESH)

    def transposed(part):
        load(part).wait()

        def one(place, carry):
            live = place < live_count[0, 0]
            for k in range(2):
                block = stage[place, k]
                block = jnp.where(live, block, jnp.zeros_like(block)).T
                block = block.reshape(groups, width, bands)
                for h in range(HALVES):
                    send[h, :, place, k * width:(k + 1) * width, :] = block[:, :, h * half:(h + 1) * half]
            return carry

        lax.fori_loop(part * quarter, (part + 1) * quarter, one, 0)

    def send_off(cs, steps):
        for c in cs:
            for r in steps:
                exchange(c, r).start()

    own_count.wait()
    transposed(0)
    pltpu.make_async_copy(maps, maps, map_sem).wait()
    landing = jnp.where(maps[0] >= 0, maps[0] * slots + maps[1], -1)
    near_map[pl.ds(me, 1)] = jnp.where(second, landing, maps[2])[None]
    pl.semaphore_wait(barrier, groups + 1)
    send_off((0,), near)
    for r in order:
        map_copy(r).start()
    send_off((0,), far)
    transposed(1)
    send_off((1,), near)
    send_off((1,), far)
    transposed(2)
    transposed(3)
    send_off((2, 3, 4), near)
    send_off((2,), far)
    pl.when(first)(functools.partial(send_off, late, far))

    for h in range(HALVES):
        own(h).start()
    for h in range(HALVES):
        own(h).wait()

    for c in range(CHUNKS):
        forward(c, 0).start()
    acc[...] = jnp.zeros_like(acc)

    def pass_on(c, steps):
        for r in steps:
            exchange(c, r).wait_recv()
            forward(c, r).start()

    def arrived(c):
        h, start, size = chunks[c]
        ref = theirs[h].at[:, pl.ds(start, size)]
        whole(ref, fsend_sem.at[h], frecv_sem.at[c], "pool", prev).wait_recv()

    for c in (0, 1, 3, 2, 4):
        near_received(c)
        for r in near:
            forward(c, r).start()
    every_map = whole(near_map.at[pl.ds(0, groups - 1)], map_send, map_recv, "ga", flipped(me, 1))
    every_map.wait_send()
    every_map.wait_recv()
    map_forward().start()
    for c in early:
        pass_on(c, far)
    map_forward().wait()
    to_scalar = pltpu.make_async_copy(far_map, slot_map, map_sem)
    to_scalar.start()
    to_scalar.wait()

    @pl.when(first)
    def _():
        pass_on(3, far)
        for c in (0, 1, 2, 3):
            far_sent(c)
        pl.semaphore_signal(gate, inc=1, device_id={"pool": succ}, device_id_type=MESH)

    @pl.when(second)
    def _():
        pl.semaphore_wait(gate, 1)
        send_off(late, far)

    def looked_up(ref, b, s):
        index = slot_map[b, 0, s]
        place = jnp.maximum(index, 0)
        block = ref[place // slots, lax.rem(place, slots)]
        return jnp.where(index >= 0, block, jnp.zeros_like(block))

    def put_ket(h, b, s, block):
        ket[b, s, :, h * bands:h * bands + half] = block
        ket[b, s, :, h * bands + half:(h + 1) * bands] = jnp.concatenate([block[width:], -block[:width]], axis=0)

    def gather_bra(h):
        def step(b, carry):
            for s in range(slots):
                picked[b, s, :, h * half:(h + 1) * half] = looked_up(mine[h], b, s)
            return carry

        lax.fori_loop(0, groups, step, 0)

    def gather_ket(h):
        def step(b, carry):
            for s in range(slots):
                put_ket(h, b, s, looked_up(theirs[h], b, s))
            return carry

        lax.fori_loop(0, groups, step, 0)

    def plain_ket(c):
        h, start, size = chunks[c]

        def step(b, carry):
            for s in range(start, start + size):
                put_ket(h, b, s, theirs[h][b, s])
            return carry

        lax.fori_loop(0, groups, step, 0)

    def multiply(bra, c, lane, row, many, column, wide, span):
        _, start, size = chunks[c]

        def step(i, carry):
            some, these = pl.ds(i * span, span), pl.ds(start, size)
            left = bra[some, these, :, pl.ds(lane, many)].reshape(span * size * depth, many)
            right = ket[some, these, :, pl.ds(column, wide)].reshape(span * size * depth, wide)
            acc[pl.ds(row, many), pl.ds(column, wide)] += lax.dot_general(
                left, right, (((0,), (0,)), ((), ())), preferred_element_type=jnp.float32
            )
            return carry

        lax.fori_loop(0, groups // span, step, 0)

    near_half = me // (groups // 2)
    far_half = 1 - near_half
    far_row = pl.multiple_of(far_half * half, half)
    near_row = pl.multiple_of(near_half * half, half)

    mates = groups // 2
    base = near_half * mates
    across = lax.rem(me + mates, groups)

    def partial_sum(side, part, j):
        dest = flipped(me, j)
        block = lax.rem(dest + side * mates, groups)
        columns = pl.ds(pl.multiple_of(part * bands, bands), bands)
        return pltpu.make_async_remote_copy(
            src_ref=acc.at[pl.ds(block * rows, rows), columns],
            dst_ref=rs.at[side, j, :, columns],
            send_sem=rs_send,
            recv_sem=rs_recv.at[side, part],
            device_id={"ga": dest},
            device_id_type=MESH,
        )

    def crossing(part):
        columns = pl.ds(part * bands, bands)
        return pltpu.make_async_remote_copy(
            src_ref=leaving.at[:, columns],
            dst_ref=entered.at[:, columns],
            send_sem=cross_send,
            recv_sem=cross_recv.at[part],
            device_id={"ga": across},
            device_id_type=MESH,
        )

    def send_partials(side, part):
        for j in range(mates - 1, 0, -1):
            partial_sum(side, part, j).start()

    def summed(side, part):
        columns = pl.ds(part * bands, bands)
        block = lax.rem(me + side * mates, groups)
        value = acc[pl.ds(pl.multiple_of(block * rows, rows), rows), columns]
        ref = rs.at[side, pl.ds(1, mates - 1), :, columns]
        whole(ref, rs_send, rs_recv.at[side, part], "ga", across).wait_recv()
        for j in range(1, mates):
            value = value + rs[side, j, :, columns]
        return value

    def cross(part):
        leaving[:, pl.ds(part * bands, bands)] = summed(1, part)
        crossing(part).start()

    low, high = near_half == 0, near_half == 1

    @pl.when(first)
    def _():
        gather_bra(0)
        for c in early:
            arrived(c)
            plain_ket(c)
            multiply(picked, c, 0, 0, half, 0, bands, groups)
        for c in late[1:]:
            pass_on(c, far)
        gather_bra(1)
        for c in early:
            multiply(picked, c, half, half, half, 0, bands, groups)
        send_partials(1, 0)
        send_partials(0, 0)
        for c in late:
            arrived(c)
            plain_ket(c)
            multiply(picked, c, far_row, far_row, half, bands, bands, groups)
        send_partials(1, 1)
        for c in late:
            multiply(picked, c, near_row, near_row, half, bands, bands, groups)
        send_partials(0, 1)
        cross(0)
        cross(1)

    @pl.when(second)
    def _():
        for c in early:
            arrived(c)
        gather_ket(0)
        for c in early:
            multiply(mine[0], c, 0, 0, half, 0, bands, groups)
        for c in late:
            arrived(c)
        pass_on(late[0], far)
        gather_ket(1)
        for c in early:
            multiply(mine[0], c, 0, 0, half, bands, bands, groups)

        def send_side(side):
            for part in range(2):
                send_partials(side, part)

        pl.when(low)(functools.partial(send_side, 0))
        pl.when(high)(functools.partial(send_side, 1))
        for c in late[1:]:
            pass_on(c, far)
        for c in late:
            multiply(mine[1], c, 0, half, half, 0, 2 * bands, groups)
        pl.when(low)(functools.partial(send_side, 1))
        pl.when(high)(functools.partial(send_side, 0))
        cross(0)
        cross(1)

    forwards_sent()
    near_sent()
    for c in late[1:]:
        far_sent(c)

    @pl.when(second)
    def _():
        for c in (0, 1, 2, 3):
            far_sent(c)

    for part in range(2):
        value = summed(0, part)
        crossing(part).wait_recv()
        value = (value + entered[:, pl.ds(part * bands, bands)]) * scale
        out[0, 0, :, pl.ds(part * half, half)] = value[:, :half]
        out[0, 1, :, pl.ds(part * half, half)] = value[:, half:]

    whole(rs.at[:, pl.ds(1, mates - 1)], rs_send, rs_recv.at[0, 0], "ga", across).wait_send()
    whole(leaving, cross_send, cross_recv.at[0], "ga", across).wait_send()


def in_one_kernel(coefficients, stick_count, dest_device, dest_slot, source_stick):
    groups = lax.axis_size("ga")
    _, slots, _, bands, waves = coefficients.shape
    depth = 2 * waves // groups
    half = bands // HALVES
    sticks = groups * slots
    rows = bands // groups
    scale = (2 * sticks * waves) ** (-0.5)
    any_space = pl.BlockSpec(memory_space=pl.ANY)
    sems = pltpu.SemaphoreType.DMA
    exchanged = pltpu.VMEM((groups, slots, depth, half), coefficients.dtype)
    return pl.pallas_call(
        functools.partial(kernel, scale),
        out_shape=pltpu.VMEM((1, 2, rows, bands), jnp.float32),
        in_specs=[any_space] * 5,
        out_specs=pl.BlockSpec(memory_space=pltpu.VMEM),
        scratch_shapes=[
            pltpu.VMEM((slots, 2, bands, waves), coefficients.dtype),
            pltpu.VMEM((HALVES, groups, slots, depth, half), coefficients.dtype),
            exchanged, exchanged, exchanged, exchanged,
            pltpu.VMEM((groups, slots, depth, bands), coefficients.dtype),
            pltpu.VMEM((groups, slots, depth, 2 * bands), coefficients.dtype),
            pltpu.VMEM((bands, 2 * bands), jnp.float32),
            pltpu.VMEM((2, groups // 2, rows, 2 * bands), jnp.float32),
            pltpu.VMEM((rows, 2 * bands), jnp.float32),
            pltpu.VMEM((rows, 2 * bands), jnp.float32),
            pltpu.VMEM((3, 1, slots), jnp.int32),
            pltpu.VMEM((groups, 1, slots), jnp.int32),
            pltpu.VMEM((groups, 1, slots), jnp.int32),
            pltpu.SMEM((1, 1), jnp.int32),
            pltpu.SMEM((groups, 1, slots), jnp.int32),
            sems((4,)), sems((HALVES,)),
            sems((CHUNKS + 1,)), sems((CHUNKS, groups // 2 + 1)), sems((HALVES,)), sems((CHUNKS,)),
            sems, sems, sems, sems, sems, sems,
            sems, sems((2, 2)), sems, sems((2,)), pltpu.SemaphoreType.REGULAR,
        ],
        compiler_params=pltpu.CompilerParams(collective_id=0, has_side_effects=True, vmem_limit_bytes=60 * 1024 * 1024),
    )(coefficients, stick_count, dest_device, dest_slot, source_stick)


def passed_along(value, axis, steps):
    count = lax.axis_size(axis)
    pairs = [(source, (source + steps) % count) for source in range(count)]
    return lax.ppermute(value, axis, pairs)


def with_collectives(coefficients, stick_count, dest_device, dest_slot, source_stick):
    groups = lax.axis_size("ga")
    slot_count = coefficients.shape[1]
    bands = coefficients.shape[3]
    plane_waves = coefficients.shape[4]
    width = plane_waves // groups
    sticks = groups * slot_count
    norm_scale = (2 * groups * slot_count * plane_waves) ** (-0.5)
    split = coefficients[0].reshape(slot_count, 2, bands, groups, width)
    split = split.transpose(3, 0, 1, 4, 2)
    mine = lax.all_to_all(split, "ga", split_axis=0, concat_axis=0, tiled=True)
    mine = mine.reshape(sticks, 2 * width * bands)
    theirs = passed_along(mine, "pool", -1)
    anchor = passed_along(source_stick[0], "pool", -1)
    slot_list = jnp.arange(slot_count, dtype=jnp.int32)
    anchor = jnp.where(slot_list < stick_count[0, 0], anchor, -1)
    anchors = lax.all_gather(anchor, "ga", tiled=True)
    placer = (anchors[:, None] == jnp.arange(sticks, dtype=jnp.int32)[None, :]).astype(jnp.bfloat16)
    ket = jnp.dot(placer, theirs, preferred_element_type=jnp.float32).astype(jnp.bfloat16)
    bra = mine.reshape(sticks, 2, width, bands)
    ket = ket.reshape(sticks, 2, width, bands)
    swapped = jnp.stack([ket[:, 1], -ket[:, 0]], axis=1)
    real_part = jnp.einsum("scgm,scgn->mn", bra, ket, preferred_element_type=jnp.float32)
    imag_part = jnp.einsum("scgm,scgn->mn", bra, swapped, preferred_element_type=jnp.float32)
    partial_value = jnp.stack([real_part, imag_part])
    owned = lax.psum_scatter(partial_value, "ga", scatter_dimension=1, tiled=True)
    return (owned * norm_scale)[None]


def local(coefficients, *rest):
    groups = lax.axis_size("ga")
    width = coefficients.shape[4] // groups
    paired = groups & (groups - 1) == 0 and lax.axis_size("pool") % 2 == 0
    if paired and width % 16 == 0 and coefficients.shape[1] % 8 == 0 and coefficients.shape[3] % 256 == 0:
        return in_one_kernel(coefficients, *rest)
    return with_collectives(coefficients, *rest)


def solution(mesh):
    return jax.shard_map(
        local,
        mesh=mesh,
        in_specs=(
            P("pool", "ga", None, None, None),
            P("pool", "ga"),
            P("pool", "ga"),
            P("pool", "ga"),
            P("pool", "ga"),
        ),
        out_specs=P("pool", None, "ga", None),
        check_vma=False,
    )
```

```python
import functools

import jax
import jax.numpy as jnp
from jax import lax
from jax.experimental import pallas as pl
from jax.experimental.pallas import tpu as pltpu
from jax.sharding import PartitionSpec as P

MESH = pl.DeviceIdType.MESH
HALVES = 2
CHUNKS = 5


def flipped(me, r):
    value = me
    bit = 1
    while bit <= r:
        if r & bit:
            value = value + bit * (1 - 2 * lax.rem(me // bit, 2))
        bit *= 2
    return value


def kernel(
    scale, coef, count, device, slot, source, out,
    stage, send, mine_a, mine_b, theirs_a, theirs_b, picked, ket, acc, rs, leaving, entered,
    maps, near_map, far_map, live_count, slot_map,
    load_sem, own_sem, send_sem, recv_sem, fsend_sem, frecv_sem,
    map_send, map_recv, fmap_send, fmap_recv, map_sem, count_sem,
    rs_send, rs_recv, cross_send, cross_recv, gate,
):
    groups, pools = lax.axis_size("ga"), lax.axis_size("pool")
    me, pool = lax.axis_index("ga"), lax.axis_index("pool")
    prev, succ = lax.rem(pool + pools - 1, pools), lax.rem(pool + 1, pools)
    slots, _, bands, waves = stage.shape
    depth = 2 * waves // groups
    width = depth // 2
    half = bands // 2
    rows = bands // groups
    mine, theirs = (mine_a, mine_b), (theirs_a, theirs_b)
    quarter = slots // 4
    chunks = [
        (0, 0, quarter), (0, quarter, quarter), (0, 2 * quarter, 2 * quarter),
        (1, 0, 3 * quarter), (1, 3 * quarter, quarter),
    ]
    early, late = (0, 1, 2), (3, 4)
    order = [1] + [r for d in range(1, groups // 2) for r in (2 * d + 1, 2 * d)]
    near = [r for r in order if r < groups // 2]
    far = [r for r in order if r >= groups // 2]
    second = lax.rem(pool, 2) == 1
    first = lax.rem(pool, 2) == 0

    def load(part):
        span = pl.ds(part * quarter, quarter)
        return pltpu.make_async_copy(coef.at[0, span], stage.at[span], load_sem.at[part])

    def own(h):
        return pltpu.make_async_copy(send.at[h, me], mine[h].at[me], own_sem.at[h])

    def exchange(c, r):
        h, start, size = chunks[c]
        dest = flipped(me, r)
        return pltpu.make_async_remote_copy(
            src_ref=send.at[h, dest, pl.ds(start, size)],
            dst_ref=mine[h].at[me, pl.ds(start, size)],
            send_sem=send_sem.at[0 if r in near else c + 1],
            recv_sem=recv_sem.at[c, 0 if r in near else r - len(near)],
            device_id={"ga": dest},
            device_id_type=MESH,
        )

    def forward(c, r):
        h, start, size = chunks[c]
        origin = flipped(me, r)
        return pltpu.make_async_remote_copy(
            src_ref=mine[h].at[origin, pl.ds(start, size)],
            dst_ref=theirs[h].at[origin, pl.ds(start, size)],
            send_sem=fsend_sem.at[h],
            recv_sem=frecv_sem.at[c],
            device_id={"pool": prev},
            device_id_type=MESH,
        )

    def whole(ref, send_one, recv_one, axis, other):
        return pltpu.make_async_remote_copy(
            src_ref=ref, dst_ref=ref, send_sem=send_one, recv_sem=recv_one,
            device_id={axis: other}, device_id_type=MESH,
        )

    def near_received(c):
        h, start, size = chunks[c]
        ref = mine[h].at[pl.ds(0, len(near)), pl.ds(start, size)]
        whole(ref, send_sem.at[0], recv_sem.at[c, 0], "ga", flipped(me, 1)).wait_recv()

    def near_sent():
        ref = send.at[:, pl.ds(0, len(near))]
        whole(ref, send_sem.at[0], recv_sem.at[0, 0], "ga", flipped(me, 1)).wait_send()

    def forwards_sent():
        for h in range(HALVES):
            whole(mine[h], fsend_sem.at[h], frecv_sem.at[0], "pool", prev).wait_send()

    def far_sent(c):
        h, start, size = chunks[c]
        ref = send.at[h, pl.ds(0, len(far)), pl.ds(start, size)]
        whole(ref, send_sem.at[c + 1], recv_sem.at[c, 0], "ga", flipped(me, 1)).wait_send()

    def map_copy(r):
        dest = flipped(me, r)
        return pltpu.make_async_remote_copy(
            src_ref=near_map.at[me],
            dst_ref=near_map.at[me],
            send_sem=map_send,
            recv_sem=map_recv,
            device_id={"ga": dest},
            device_id_type=MESH,
        )

    def map_forward():
        return pltpu.make_async_remote_copy(
            src_ref=near_map,
            dst_ref=far_map,
            send_sem=fmap_send,
            recv_sem=fmap_recv,
            device_id={"pool": prev},
            device_id_type=MESH,
        )

    own_count = pltpu.make_async_copy(count, live_count, count_sem)
    own_count.start()
    for part in range(4):
        load(part).start()
    own_maps = [
        pltpu.make_async_copy(ref, maps.at[n], map_sem)
        for n, ref in enumerate((device, slot, source))
    ]
    for copy in own_maps:
        copy.start()

    barrier = pltpu.get_barrier_semaphore()
    for r in order:
        pl.semaphore_signal(barrier, inc=1, device_id={"ga": flipped(me, r)}, device_id_type=MESH)
    for other in (prev, succ):
        pl.semaphore_signal(barrier, inc=1, device_id={"pool": other}, device_id_type=MESH)

    def transposed(part):
        load(part).wait()

        def one(place, carry):
            live = place < live_count[0, 0]
            for k in range(2):
                block = stage[place, k]
                block = jnp.where(live, block, jnp.zeros_like(block)).T
                block = block.reshape(groups, width, bands)
                for h in range(HALVES):
                    send[h, :, place, k * width:(k + 1) * width, :] = block[:, :, h * half:(h + 1) * half]
            return carry

        lax.fori_loop(part * quarter, (part + 1) * quarter, one, 0)

    def send_off(cs, steps):
        for c in cs:
            for r in steps:
                exchange(c, r).start()

    own_count.wait()
    transposed(0)
    pltpu.make_async_copy(maps, maps, map_sem).wait()
    landing = jnp.where(maps[0] >= 0, maps[0] * slots + maps[1], -1)
    near_map[pl.ds(me, 1)] = jnp.where(second, landing, maps[2])[None]
    pl.semaphore_wait(barrier, groups + 1)
    send_off((0,), near)
    for r in order:
        map_copy(r).start()
    send_off((0,), far)
    transposed(1)
    send_off((1,), near)
    send_off((1,), far)
    transposed(2)
    transposed(3)
    send_off((2, 3, 4), near)
    send_off((2,), far)
    pl.when(first)(functools.partial(send_off, late, far))

    for h in range(HALVES):
        own(h).start()
    for h in range(HALVES):
        own(h).wait()

    for c in range(CHUNKS):
        forward(c, 0).start()
    acc[...] = jnp.zeros_like(acc)

    def pass_on(c, steps):
        for r in steps:
            exchange(c, r).wait_recv()
            forward(c, r).start()

    def arrived(c):
        h, start, size = chunks[c]
        ref = theirs[h].at[:, pl.ds(start, size)]
        whole(ref, fsend_sem.at[h], frecv_sem.at[c], "pool", prev).wait_recv()

    for c in (0, 1, 3, 2, 4):
        near_received(c)
        for r in near:
            forward(c, r).start()
    every_map = whole(near_map.at[pl.ds(0, groups - 1)], map_send, map_recv, "ga", flipped(me, 1))
    every_map.wait_send()
    every_map.wait_recv()
    map_forward().start()
    for c in early:
        pass_on(c, far)
    map_forward().wait()
    to_scalar = pltpu.make_async_copy(far_map, slot_map, map_sem)
    to_scalar.start()
    to_scalar.wait()

    @pl.when(first)
    def _():
        pass_on(3, far)
        for c in (0, 1, 2, 3):
            far_sent(c)
        pl.semaphore_signal(gate, inc=1, device_id={"pool": succ}, device_id_type=MESH)

    @pl.when(second)
    def _():
        pl.semaphore_wait(gate, 1)
        send_off(late, far)

    def looked_up(ref, b, s):
        index = slot_map[b, 0, s]
        place = jnp.maximum(index, 0)
        block = ref[place // slots, lax.rem(place, slots)]
        return jnp.where(index >= 0, block, jnp.zeros_like(block))

    def put_ket(h, b, s, block):
        ket[b, s, :, h * bands:h * bands + half] = block
        ket[b, s, :, h * bands + half:(h + 1) * bands] = jnp.concatenate([block[width:], -block[:width]], axis=0)

    def gather_bra(h):
        def step(b, carry):
            for s in range(slots):
                picked[b, s, :, h * half:(h + 1) * half] = looked_up(mine[h], b, s)
            return carry

        lax.fori_loop(0, groups, step, 0)

    def gather_ket(h):
        def step(b, carry):
            for s in range(slots):
                put_ket(h, b, s, looked_up(theirs[h], b, s))
            return carry

        lax.fori_loop(0, groups, step, 0)

    def plain_ket(c):
        h, start, size = chunks[c]

        def step(b, carry):
            for s in range(start, start + size):
                put_ket(h, b, s, theirs[h][b, s])
            return carry

        lax.fori_loop(0, groups, step, 0)

    def multiply(bra, c, lane, row, many, column, wide, span):
        _, start, size = chunks[c]

        def step(i, carry):
            some, these = pl.ds(i * span, span), pl.ds(start, size)
            left = bra[some, these, :, pl.ds(lane, many)].reshape(span * size * depth, many)
            right = ket[some, these, :, pl.ds(column, wide)].reshape(span * size * depth, wide)
            acc[pl.ds(row, many), pl.ds(column, wide)] += lax.dot_general(
                left, right, (((0,), (0,)), ((), ())), preferred_element_type=jnp.float32
            )
            return carry

        lax.fori_loop(0, groups // span, step, 0)

    near_half = me // (groups // 2)
    far_half = 1 - near_half
    far_row = pl.multiple_of(far_half * half, half)
    near_row = pl.multiple_of(near_half * half, half)

    mates = groups // 2
    base = near_half * mates
    across = lax.rem(me + mates, groups)

    def partial_sum(side, part, j):
        dest = flipped(me, j)
        block = lax.rem(dest + side * mates, groups)
        columns = pl.ds(pl.multiple_of(part * bands, bands), bands)
        return pltpu.make_async_remote_copy(
            src_ref=acc.at[pl.ds(block * rows, rows), columns],
            dst_ref=rs.at[side, j, :, columns],
            send_sem=rs_send,
            recv_sem=rs_recv.at[side, part],
            device_id={"ga": dest},
            device_id_type=MESH,
        )

    def crossing(part):
        columns = pl.ds(part * bands, bands)
        return pltpu.make_async_remote_copy(
            src_ref=leaving.at[:, columns],
            dst_ref=entered.at[:, columns],
            send_sem=cross_send,
            recv_sem=cross_recv.at[part],
            device_id={"ga": across},
            device_id_type=MESH,
        )

    def send_partials(side, part):
        for j in range(mates - 1, 0, -1):
            partial_sum(side, part, j).start()

    def summed(side, part):
        columns = pl.ds(part * bands, bands)
        block = lax.rem(me + side * mates, groups)
        value = acc[pl.ds(pl.multiple_of(block * rows, rows), rows), columns]
        ref = rs.at[side, pl.ds(1, mates - 1), :, columns]
        whole(ref, rs_send, rs_recv.at[side, part], "ga", across).wait_recv()
        for j in range(1, mates):
            value = value + rs[side, j, :, columns]
        return value

    def cross(part):
        leaving[:, pl.ds(part * bands, bands)] = summed(1, part)
        crossing(part).start()

    low, high = near_half == 0, near_half == 1

    @pl.when(first)
    def _():
        gather_bra(0)
        for c in early:
            arrived(c)
            plain_ket(c)
            multiply(picked, c, 0, 0, half, 0, bands, groups)
        for c in late[1:]:
            pass_on(c, far)
        gather_bra(1)
        for c in early:
            multiply(picked, c, half, half, half, 0, bands, groups)
        send_partials(1, 0)
        send_partials(0, 0)
        for c in late:
            arrived(c)
            plain_ket(c)
            multiply(picked, c, far_row, far_row, half, bands, bands, groups)
        send_partials(1, 1)
        cross(0)
        for c in late:
            multiply(picked, c, near_row, near_row, half, bands, bands, groups)
        send_partials(0, 1)
        cross(1)

    @pl.when(second)
    def _():
        for c in early:
            arrived(c)
        gather_ket(0)
        for c in early:
            multiply(mine[0], c, 0, 0, half, 0, bands, groups)
        for c in late:
            arrived(c)
        pass_on(late[0], far)
        gather_ket(1)
        for c in early:
            multiply(mine[0], c, 0, 0, half, bands, bands, groups)

        def send_side(side):
            for part in range(2):
                send_partials(side, part)

        pl.when(low)(functools.partial(send_side, 0))
        pl.when(high)(functools.partial(send_side, 1))
        for c in late[1:]:
            pass_on(c, far)
        for c in late:
            multiply(mine[1], c, 0, half, half, 0, 2 * bands, groups)
        pl.when(low)(functools.partial(send_side, 1))
        pl.when(high)(functools.partial(send_side, 0))
        cross(0)
        cross(1)

    forwards_sent()
    near_sent()
    for c in late[1:]:
        far_sent(c)

    @pl.when(second)
    def _():
        for c in (0, 1, 2, 3):
            far_sent(c)

    for part in range(2):
        value = summed(0, part)
        crossing(part).wait_recv()
        value = (value + entered[:, pl.ds(part * bands, bands)]) * scale
        out[0, 0, :, pl.ds(part * half, half)] = value[:, :half]
        out[0, 1, :, pl.ds(part * half, half)] = value[:, half:]

    whole(rs.at[:, pl.ds(1, mates - 1)], rs_send, rs_recv.at[0, 0], "ga", across).wait_send()
    whole(leaving, cross_send, cross_recv.at[0], "ga", across).wait_send()


def in_one_kernel(coefficients, stick_count, dest_device, dest_slot, source_stick):
    groups = lax.axis_size("ga")
    _, slots, _, bands, waves = coefficients.shape
    depth = 2 * waves // groups
    half = bands // HALVES
    sticks = groups * slots
    rows = bands // groups
    scale = (2 * sticks * waves) ** (-0.5)
    any_space = pl.BlockSpec(memory_space=pl.ANY)
    sems = pltpu.SemaphoreType.DMA
    exchanged = pltpu.VMEM((groups, slots, depth, half), coefficients.dtype)
    return pl.pallas_call(
        functools.partial(kernel, scale),
        out_shape=pltpu.VMEM((1, 2, rows, bands), jnp.float32),
        in_specs=[any_space] * 5,
        out_specs=pl.BlockSpec(memory_space=pltpu.VMEM),
        scratch_shapes=[
            pltpu.VMEM((slots, 2, bands, waves), coefficients.dtype),
            pltpu.VMEM((HALVES, groups, slots, depth, half), coefficients.dtype),
            exchanged, exchanged, exchanged, exchanged,
            pltpu.VMEM((groups, slots, depth, bands), coefficients.dtype),
            pltpu.VMEM((groups, slots, depth, 2 * bands), coefficients.dtype),
            pltpu.VMEM((bands, 2 * bands), jnp.float32),
            pltpu.VMEM((2, groups // 2, rows, 2 * bands), jnp.float32),
            pltpu.VMEM((rows, 2 * bands), jnp.float32),
            pltpu.VMEM((rows, 2 * bands), jnp.float32),
            pltpu.VMEM((3, 1, slots), jnp.int32),
            pltpu.VMEM((groups, 1, slots), jnp.int32),
            pltpu.VMEM((groups, 1, slots), jnp.int32),
            pltpu.SMEM((1, 1), jnp.int32),
            pltpu.SMEM((groups, 1, slots), jnp.int32),
            sems((4,)), sems((HALVES,)),
            sems((CHUNKS + 1,)), sems((CHUNKS, groups // 2 + 1)), sems((HALVES,)), sems((CHUNKS,)),
            sems, sems, sems, sems, sems, sems,
            sems, sems((2, 2)), sems, sems((2,)), pltpu.SemaphoreType.REGULAR,
        ],
        compiler_params=pltpu.CompilerParams(collective_id=0, has_side_effects=True, vmem_limit_bytes=60 * 1024 * 1024),
    )(coefficients, stick_count, dest_device, dest_slot, source_stick)


def passed_along(value, axis, steps):
    count = lax.axis_size(axis)
    pairs = [(source, (source + steps) % count) for source in range(count)]
    return lax.ppermute(value, axis, pairs)


def with_collectives(coefficients, stick_count, dest_device, dest_slot, source_stick):
    groups = lax.axis_size("ga")
    slot_count = coefficients.shape[1]
    bands = coefficients.shape[3]
    plane_waves = coefficients.shape[4]
    width = plane_waves // groups
    sticks = groups * slot_count
    norm_scale = (2 * groups * slot_count * plane_waves) ** (-0.5)
    split = coefficients[0].reshape(slot_count, 2, bands, groups, width)
    split = split.transpose(3, 0, 1, 4, 2)
    mine = lax.all_to_all(split, "ga", split_axis=0, concat_axis=0, tiled=True)
    mine = mine.reshape(sticks, 2 * width * bands)
    theirs = passed_along(mine, "pool", -1)
    anchor = passed_along(source_stick[0], "pool", -1)
    slot_list = jnp.arange(slot_count, dtype=jnp.int32)
    anchor = jnp.where(slot_list < stick_count[0, 0], anchor, -1)
    anchors = lax.all_gather(anchor, "ga", tiled=True)
    placer = (anchors[:, None] == jnp.arange(sticks, dtype=jnp.int32)[None, :]).astype(jnp.bfloat16)
    ket = jnp.dot(placer, theirs, preferred_element_type=jnp.float32).astype(jnp.bfloat16)
    bra = mine.reshape(sticks, 2, width, bands)
    ket = ket.reshape(sticks, 2, width, bands)
    swapped = jnp.stack([ket[:, 1], -ket[:, 0]], axis=1)
    real_part = jnp.einsum("scgm,scgn->mn", bra, ket, preferred_element_type=jnp.float32)
    imag_part = jnp.einsum("scgm,scgn->mn", bra, swapped, preferred_element_type=jnp.float32)
    partial_value = jnp.stack([real_part, imag_part])
    owned = lax.psum_scatter(partial_value, "ga", scatter_dimension=1, tiled=True)
    return (owned * norm_scale)[None]


def local(coefficients, *rest):
    groups = lax.axis_size("ga")
    width = coefficients.shape[4] // groups
    paired = groups & (groups - 1) == 0 and lax.axis_size("pool") % 2 == 0
    if paired and width % 16 == 0 and coefficients.shape[1] % 8 == 0 and coefficients.shape[3] % 256 == 0:
        return in_one_kernel(coefficients, *rest)
    return with_collectives(coefficients, *rest)


def solution(mesh):
    return jax.shard_map(
        local,
        mesh=mesh,
        in_specs=(
            P("pool", "ga", None, None, None),
            P("pool", "ga"),
            P("pool", "ga"),
            P("pool", "ga"),
            P("pool", "ga"),
        ),
        out_specs=P("pool", None, "ga", None),
        check_vma=False,
    )
```

```python
import functools

import jax
import jax.numpy as jnp
from jax import lax
from jax.experimental import pallas as pl
from jax.experimental.pallas import tpu as pltpu
from jax.sharding import PartitionSpec as P

MESH = pl.DeviceIdType.MESH
HALVES = 2
CHUNKS = 5


def flipped(me, r):
    value = me
    bit = 1
    while bit <= r:
        if r & bit:
            value = value + bit * (1 - 2 * lax.rem(me // bit, 2))
        bit *= 2
    return value


def kernel(
    scale, coef, count, device, slot, source, out,
    stage, send, mine_a, mine_b, theirs_a, theirs_b, picked, ket, acc, rs, leaving, entered,
    maps, near_map, far_map, live_count, slot_map,
    load_sem, own_sem, send_sem, recv_sem, fsend_sem, frecv_sem,
    map_send, map_recv, fmap_send, fmap_recv, map_sem, count_sem,
    rs_send, rs_recv, cross_send, cross_recv, gate,
):
    groups, pools = lax.axis_size("ga"), lax.axis_size("pool")
    me, pool = lax.axis_index("ga"), lax.axis_index("pool")
    prev, succ = lax.rem(pool + pools - 1, pools), lax.rem(pool + 1, pools)
    slots, _, bands, waves = stage.shape
    depth = 2 * waves // groups
    width = depth // 2
    half = bands // 2
    rows = bands // groups
    mine, theirs = (mine_a, mine_b), (theirs_a, theirs_b)
    quarter = slots // 4
    chunks = [
        (0, 0, quarter), (0, quarter, quarter), (0, 2 * quarter, 2 * quarter),
        (1, 0, 3 * quarter), (1, 3 * quarter, quarter),
    ]
    early, late = (0, 1, 2), (3, 4)
    order = [1] + [r for d in range(1, groups // 2) for r in (2 * d + 1, 2 * d)]
    near = [r for r in order if r < groups // 2]
    far = [r for r in order if r >= groups // 2]
    second = lax.rem(pool, 2) == 1
    first = lax.rem(pool, 2) == 0

    def load(part):
        span = pl.ds(part * quarter, quarter)
        return pltpu.make_async_copy(coef.at[0, span], stage.at[span], load_sem.at[part])

    def own(h):
        return pltpu.make_async_copy(send.at[h, me], mine[h].at[me], own_sem.at[h])

    def exchange(c, r):
        h, start, size = chunks[c]
        dest = flipped(me, r)
        return pltpu.make_async_remote_copy(
            src_ref=send.at[h, dest, pl.ds(start, size)],
            dst_ref=mine[h].at[me, pl.ds(start, size)],
            send_sem=send_sem.at[0 if r in near else c + 1],
            recv_sem=recv_sem.at[c, 0 if r in near else r - len(near)],
            device_id={"ga": dest},
            device_id_type=MESH,
        )

    def forward(c, r):
        h, start, size = chunks[c]
        origin = flipped(me, r)
        return pltpu.make_async_remote_copy(
            src_ref=mine[h].at[origin, pl.ds(start, size)],
            dst_ref=theirs[h].at[origin, pl.ds(start, size)],
            send_sem=fsend_sem.at[h],
            recv_sem=frecv_sem.at[c],
            device_id={"pool": prev},
            device_id_type=MESH,
        )

    def whole(ref, send_one, recv_one, axis, other):
        return pltpu.make_async_remote_copy(
            src_ref=ref, dst_ref=ref, send_sem=send_one, recv_sem=recv_one,
            device_id={axis: other}, device_id_type=MESH,
        )

    def near_received(c):
        h, start, size = chunks[c]
        ref = mine[h].at[pl.ds(0, len(near)), pl.ds(start, size)]
        whole(ref, send_sem.at[0], recv_sem.at[c, 0], "ga", flipped(me, 1)).wait_recv()

    def near_sent():
        ref = send.at[:, pl.ds(0, len(near))]
        whole(ref, send_sem.at[0], recv_sem.at[0, 0], "ga", flipped(me, 1)).wait_send()

    def forwards_sent():
        for h in range(HALVES):
            whole(mine[h], fsend_sem.at[h], frecv_sem.at[0], "pool", prev).wait_send()

    def far_sent(c):
        h, start, size = chunks[c]
        ref = send.at[h, pl.ds(0, len(far)), pl.ds(start, size)]
        whole(ref, send_sem.at[c + 1], recv_sem.at[c, 0], "ga", flipped(me, 1)).wait_send()

    def map_copy(r):
        dest = flipped(me, r)
        return pltpu.make_async_remote_copy(
            src_ref=near_map.at[me],
            dst_ref=near_map.at[me],
            send_sem=map_send,
            recv_sem=map_recv,
            device_id={"ga": dest},
            device_id_type=MESH,
        )

    def map_forward():
        return pltpu.make_async_remote_copy(
            src_ref=near_map,
            dst_ref=far_map,
            send_sem=fmap_send,
            recv_sem=fmap_recv,
            device_id={"pool": prev},
            device_id_type=MESH,
        )

    own_count = pltpu.make_async_copy(count, live_count, count_sem)
    own_count.start()
    for part in range(4):
        load(part).start()
    own_maps = [
        pltpu.make_async_copy(ref, maps.at[n], map_sem)
        for n, ref in enumerate((device, slot, source))
    ]
    for copy in own_maps:
        copy.start()

    barrier = pltpu.get_barrier_semaphore()
    for r in order:
        pl.semaphore_signal(barrier, inc=1, device_id={"ga": flipped(me, r)}, device_id_type=MESH)
    for other in (prev, succ):
        pl.semaphore_signal(barrier, inc=1, device_id={"pool": other}, device_id_type=MESH)

    def transposed(part):
        load(part).wait()

        def one(place, carry):
            live = place < live_count[0, 0]
            for k in range(2):
                block = stage[place, k]
                block = jnp.where(live, block, jnp.zeros_like(block)).T
                block = block.reshape(groups, width, bands)
                for h in range(HALVES):
                    send[h, :, place, k * width:(k + 1) * width, :] = block[:, :, h * half:(h + 1) * half]
            return carry

        lax.fori_loop(part * quarter, (part + 1) * quarter, one, 0)

    def send_off(cs, steps):
        for c in cs:
            for r in steps:
                exchange(c, r).start()

    own_count.wait()
    transposed(0)
    pltpu.make_async_copy(maps, maps, map_sem).wait()
    landing = jnp.where(maps[0] >= 0, maps[0] * slots + maps[1], -1)
    near_map[pl.ds(me, 1)] = jnp.where(second, landing, maps[2])[None]
    pl.semaphore_wait(barrier, groups + 1)
    send_off((0,), near)
    for r in order:
        map_copy(r).start()
    send_off((0,), far)
    transposed(1)
    send_off((1,), near)
    send_off((1,), far)
    transposed(2)
    transposed(3)
    send_off((2, 3, 4), near)
    send_off((2,), far)
    pl.when(first)(functools.partial(send_off, late, far))

    for h in range(HALVES):
        own(h).start()
    for h in range(HALVES):
        own(h).wait()

    for c in range(CHUNKS):
        forward(c, 0).start()
    acc[...] = jnp.zeros_like(acc)

    def pass_on(c, steps):
        for r in steps:
            exchange(c, r).wait_recv()
            forward(c, r).start()

    def arrived(c):
        h, start, size = chunks[c]
        ref = theirs[h].at[:, pl.ds(start, size)]
        whole(ref, fsend_sem.at[h], frecv_sem.at[c], "pool", prev).wait_recv()

    for c in (0, 1, 3, 2, 4):
        near_received(c)
        for r in near:
            forward(c, r).start()
    every_map = whole(near_map.at[pl.ds(0, groups - 1)], map_send, map_recv, "ga", flipped(me, 1))
    every_map.wait_send()
    every_map.wait_recv()
    map_forward().start()
    for c in early:
        pass_on(c, far)
    map_forward().wait()
    to_scalar = pltpu.make_async_copy(far_map, slot_map, map_sem)
    to_scalar.start()
    to_scalar.wait()

    @pl.when(first)
    def _():
        pass_on(3, far)
        for c in (0, 1, 2, 3):
            far_sent(c)
        pl.semaphore_signal(gate, inc=1, device_id={"pool": succ}, device_id_type=MESH)

    @pl.when(second)
    def _():
        pl.semaphore_wait(gate, 1)
        send_off(late, far)

    def looked_up(ref, b, s):
        index = slot_map[b, 0, s]
        place = jnp.maximum(index, 0)
        block = ref[place // slots, lax.rem(place, slots)]
        return jnp.where(index >= 0, block, jnp.zeros_like(block))

    def put_ket(h, b, s, block):
        ket[b, s, :, h * bands:h * bands + half] = block
        ket[b, s, :, h * bands + half:(h + 1) * bands] = jnp.concatenate([block[width:], -block[:width]], axis=0)

    def gather_bra(h):
        def step(b, carry):
            for s in range(slots):
                picked[b, s, :, h * half:(h + 1) * half] = looked_up(mine[h], b, s)
            return carry

        lax.fori_loop(0, groups, step, 0)

    def gather_ket(h):
        def step(b, carry):
            for s in range(slots):
                put_ket(h, b, s, looked_up(theirs[h], b, s))
            return carry

        lax.fori_loop(0, groups, step, 0)

    def plain_ket(c):
        h, start, size = chunks[c]

        def step(b, carry):
            for s in range(start, start + size):
                put_ket(h, b, s, theirs[h][b, s])
            return carry

        lax.fori_loop(0, groups, step, 0)

    def multiply(bra, c, lane, row, many, column, wide, span):
        _, start, size = chunks[c]

        def step(i, carry):
            some, these = pl.ds(i * span, span), pl.ds(start, size)
            left = bra[some, these, :, pl.ds(lane, many)].reshape(span * size * depth, many)
            right = ket[some, these, :, pl.ds(column, wide)].reshape(span * size * depth, wide)
            acc[pl.ds(row, many), pl.ds(column, wide)] += lax.dot_general(
                left, right, (((0,), (0,)), ((), ())), preferred_element_type=jnp.float32
            )
            return carry

        lax.fori_loop(0, groups // span, step, 0)

    near_half = me // (groups // 2)
    far_half = 1 - near_half
    far_row = pl.multiple_of(far_half * half, half)
    near_row = pl.multiple_of(near_half * half, half)

    mates = groups // 2
    base = near_half * mates
    across = lax.rem(me + mates, groups)

    def partial_sum(side, part, j):
        dest = flipped(me, j)
        block = lax.rem(dest + side * mates, groups)
        columns = pl.ds(pl.multiple_of(part * bands, bands), bands)
        return pltpu.make_async_remote_copy(
            src_ref=acc.at[pl.ds(block * rows, rows), columns],
            dst_ref=rs.at[side, j, :, columns],
            send_sem=rs_send,
            recv_sem=rs_recv.at[side, part],
            device_id={"ga": dest},
            device_id_type=MESH,
        )

    def crossing(part):
        columns = pl.ds(part * bands, bands)
        return pltpu.make_async_remote_copy(
            src_ref=leaving.at[:, columns],
            dst_ref=entered.at[:, columns],
            send_sem=cross_send,
            recv_sem=cross_recv.at[part],
            device_id={"ga": across},
            device_id_type=MESH,
        )

    def send_partials(side, part):
        for j in range(mates - 1, 0, -1):
            partial_sum(side, part, j).start()

    def summed(side, part):
        columns = pl.ds(part * bands, bands)
        block = lax.rem(me + side * mates, groups)
        value = acc[pl.ds(pl.multiple_of(block * rows, rows), rows), columns]
        ref = rs.at[side, pl.ds(1, mates - 1), :, columns]
        whole(ref, rs_send, rs_recv.at[side, part], "ga", across).wait_recv()
        for j in range(1, mates):
            value = value + rs[side, j, :, columns]
        return value

    def cross(part):
        leaving[:, pl.ds(part * bands, bands)] = summed(1, part)
        crossing(part).start()

    low, high = near_half == 0, near_half == 1

    @pl.when(first)
    def _():
        gather_bra(0)
        for c in early:
            arrived(c)
            plain_ket(c)
            multiply(picked, c, 0, 0, half, 0, bands, groups)
        for c in late[1:]:
            pass_on(c, far)
        gather_bra(1)
        for c in early:
            multiply(picked, c, half, half, half, 0, bands, groups)
        send_partials(1, 0)
        send_partials(0, 0)
        for c in late[:-1]:
            arrived(c)
            plain_ket(c)
            multiply(picked, c, 0, 0, bands, bands, bands, groups)
        for c in late[-1:]:
            arrived(c)
            plain_ket(c)
            multiply(picked, c, far_row, far_row, half, bands, bands, groups)
        send_partials(1, 1)
        cross(0)
        for c in late[-1:]:
            multiply(picked, c, near_row, near_row, half, bands, bands, groups)
        send_partials(0, 1)
        cross(1)

    @pl.when(second)
    def _():
        for c in early:
            arrived(c)
        gather_ket(0)
        for c in early:
            multiply(mine[0], c, 0, 0, half, 0, bands, groups)
        for c in late:
            arrived(c)
        pass_on(late[0], far)
        gather_ket(1)
        for c in early:
            multiply(mine[0], c, 0, 0, half, bands, bands, groups)

        def send_side(side):
            for part in range(2):
                send_partials(side, part)

        pl.when(low)(functools.partial(send_side, 0))
        pl.when(high)(functools.partial(send_side, 1))
        for c in late[1:]:
            pass_on(c, far)
        for c in late:
            multiply(mine[1], c, 0, half, half, 0, 2 * bands, groups)
        pl.when(low)(functools.partial(send_side, 1))
        pl.when(high)(functools.partial(send_side, 0))
        cross(0)
        cross(1)

    forwards_sent()
    near_sent()
    for c in late[1:]:
        far_sent(c)

    @pl.when(second)
    def _():
        for c in (0, 1, 2, 3):
            far_sent(c)

    for part in range(2):
        value = summed(0, part)
        crossing(part).wait_recv()
        value = (value + entered[:, pl.ds(part * bands, bands)]) * scale
        out[0, 0, :, pl.ds(part * half, half)] = value[:, :half]
        out[0, 1, :, pl.ds(part * half, half)] = value[:, half:]

    whole(rs.at[:, pl.ds(1, mates - 1)], rs_send, rs_recv.at[0, 0], "ga", across).wait_send()
    whole(leaving, cross_send, cross_recv.at[0], "ga", across).wait_send()


def in_one_kernel(coefficients, stick_count, dest_device, dest_slot, source_stick):
    groups = lax.axis_size("ga")
    _, slots, _, bands, waves = coefficients.shape
    depth = 2 * waves // groups
    half = bands // HALVES
    sticks = groups * slots
    rows = bands // groups
    scale = (2 * sticks * waves) ** (-0.5)
    any_space = pl.BlockSpec(memory_space=pl.ANY)
    sems = pltpu.SemaphoreType.DMA
    exchanged = pltpu.VMEM((groups, slots, depth, half), coefficients.dtype)
    return pl.pallas_call(
        functools.partial(kernel, scale),
        out_shape=pltpu.VMEM((1, 2, rows, bands), jnp.float32),
        in_specs=[any_space] * 5,
        out_specs=pl.BlockSpec(memory_space=pltpu.VMEM),
        scratch_shapes=[
            pltpu.VMEM((slots, 2, bands, waves), coefficients.dtype),
            pltpu.VMEM((HALVES, groups, slots, depth, half), coefficients.dtype),
            exchanged, exchanged, exchanged, exchanged,
            pltpu.VMEM((groups, slots, depth, bands), coefficients.dtype),
            pltpu.VMEM((groups, slots, depth, 2 * bands), coefficients.dtype),
            pltpu.VMEM((bands, 2 * bands), jnp.float32),
            pltpu.VMEM((2, groups // 2, rows, 2 * bands), jnp.float32),
            pltpu.VMEM((rows, 2 * bands), jnp.float32),
            pltpu.VMEM((rows, 2 * bands), jnp.float32),
            pltpu.VMEM((3, 1, slots), jnp.int32),
            pltpu.VMEM((groups, 1, slots), jnp.int32),
            pltpu.VMEM((groups, 1, slots), jnp.int32),
            pltpu.SMEM((1, 1), jnp.int32),
            pltpu.SMEM((groups, 1, slots), jnp.int32),
            sems((4,)), sems((HALVES,)),
            sems((CHUNKS + 1,)), sems((CHUNKS, groups // 2 + 1)), sems((HALVES,)), sems((CHUNKS,)),
            sems, sems, sems, sems, sems, sems,
            sems, sems((2, 2)), sems, sems((2,)), pltpu.SemaphoreType.REGULAR,
        ],
        compiler_params=pltpu.CompilerParams(collective_id=0, has_side_effects=True, vmem_limit_bytes=60 * 1024 * 1024),
    )(coefficients, stick_count, dest_device, dest_slot, source_stick)


def passed_along(value, axis, steps):
    count = lax.axis_size(axis)
    pairs = [(source, (source + steps) % count) for source in range(count)]
    return lax.ppermute(value, axis, pairs)


def with_collectives(coefficients, stick_count, dest_device, dest_slot, source_stick):
    groups = lax.axis_size("ga")
    slot_count = coefficients.shape[1]
    bands = coefficients.shape[3]
    plane_waves = coefficients.shape[4]
    width = plane_waves // groups
    sticks = groups * slot_count
    norm_scale = (2 * groups * slot_count * plane_waves) ** (-0.5)
    split = coefficients[0].reshape(slot_count, 2, bands, groups, width)
    split = split.transpose(3, 0, 1, 4, 2)
    mine = lax.all_to_all(split, "ga", split_axis=0, concat_axis=0, tiled=True)
    mine = mine.reshape(sticks, 2 * width * bands)
    theirs = passed_along(mine, "pool", -1)
    anchor = passed_along(source_stick[0], "pool", -1)
    slot_list = jnp.arange(slot_count, dtype=jnp.int32)
    anchor = jnp.where(slot_list < stick_count[0, 0], anchor, -1)
    anchors = lax.all_gather(anchor, "ga", tiled=True)
    placer = (anchors[:, None] == jnp.arange(sticks, dtype=jnp.int32)[None, :]).astype(jnp.bfloat16)
    ket = jnp.dot(placer, theirs, preferred_element_type=jnp.float32).astype(jnp.bfloat16)
    bra = mine.reshape(sticks, 2, width, bands)
    ket = ket.reshape(sticks, 2, width, bands)
    swapped = jnp.stack([ket[:, 1], -ket[:, 0]], axis=1)
    real_part = jnp.einsum("scgm,scgn->mn", bra, ket, preferred_element_type=jnp.float32)
    imag_part = jnp.einsum("scgm,scgn->mn", bra, swapped, preferred_element_type=jnp.float32)
    partial_value = jnp.stack([real_part, imag_part])
    owned = lax.psum_scatter(partial_value, "ga", scatter_dimension=1, tiled=True)
    return (owned * norm_scale)[None]


def local(coefficients, *rest):
    groups = lax.axis_size("ga")
    width = coefficients.shape[4] // groups
    paired = groups & (groups - 1) == 0 and lax.axis_size("pool") % 2 == 0
    if paired and width % 16 == 0 and coefficients.shape[1] % 8 == 0 and coefficients.shape[3] % 256 == 0:
        return in_one_kernel(coefficients, *rest)
    return with_collectives(coefficients, *rest)


def solution(mesh):
    return jax.shard_map(
        local,
        mesh=mesh,
        in_specs=(
            P("pool", "ga", None, None, None),
            P("pool", "ga"),
            P("pool", "ga"),
            P("pool", "ga"),
            P("pool", "ga"),
        ),
        out_specs=P("pool", None, "ga", None),
        check_vma=False,
    )
```
